256 devices in a mesh: unit: 4 (over y), bank: 4 (over x), zero: 16 (over z, core).
Axes of the slice: x: 4, y: 4, z: 8, core: 2. Of those that a mesh axis runs over, the one named last changes fastest.
Arguments:
- train_down: float32 [256, 1024, 2048], P(('unit', 'bank'), None, 'zero'), parts along dimension 0, may hold values from -0.25 to 0.25
- router_weight: float32 [8192, 64], P(('unit', 'zero'), 'bank'), parts along dimension 0, may hold values from -0.125 to 0.125
- router_gain: float32 [8192], P(('unit', 'zero')), parts along dimension 0, may hold values from 0.25 to 1.75
Outputs:
- ready_down: bfloat16 [256, 1024, 2048], P(('unit', 'bank'), 'zero'), parts along dimension 0
- scale_down: float32 [256, 1024], P(('unit', 'bank'), 'zero'), parts along dimension 0
- serve_router: bfloat16 [8192, 64], P('unit'), parts along dimension 0
The draws below stay inside these ranges and needn't reach their ends.
There are 4 independent parts, one for each index of `unit`. The reference program is written for one: setup_inputs(seed, part) draws one part's arguments, and reference() takes and returns one part's arrays. A program takes and returns all parts, laid end to end along the dimension named above; each array names one. Nothing has to cross between parts.
All inputs are finite; a program needn't handle non-finite values.
Results may differ from the reference program's by a relative error of at most 0.001.
Values may be sent and summed in bfloat16 or wider, within the bound.
A program may use at most 128 MiB of HBM per device.

```python
import jax
import jax.numpy as jnp

EXPERTS = 64
D_MODEL = 2048
D_EXPERT = 1024


def with_spikes(drawn, own_key, source, target, parts, factor):
    owner, partner = [(jnp.arange(drawn.shape[axis_at]) // (drawn.shape[axis_at] // parts)).reshape([-1 if axis == axis_at else 1 for axis in range(drawn.ndim)]) for axis_at in (source, target)]
    chosen = jax.random.permutation(own_key, parts)[partner]
    strong = (owner == chosen) | (owner == (partner + parts // 2) % parts)
    return jnp.where(strong, factor * drawn, drawn)


def levels(rng, extent, split, smallest, high):
    gain = 1.0
    for position, shards_of in split:
        draws = jax.random.uniform(jax.random.fold_in(jax.random.fold_in(rng, 6), position), (shards_of,), jnp.float32, smallest / len(split), high / len(split))
        gain = gain * jnp.repeat(jnp.exp(draws), extent[position] // shards_of).reshape((-1,) + (1,) * (len(extent) - 1 - position))
    return gain


def gaussian(own_key, dims, spread, most, shards=(), dtype=jnp.bfloat16):
    array = jax.random.normal(own_key, dims, jnp.float32) * spread
    if len(shards) > 0:
        array = levels(own_key, dims, shards, -0.22, 0.18) * array
    return jnp.clip(array, min=-most, max=most).astype(dtype)


def bell_draw_with(stream_key, extent, width, bound, pieces, heavy, held_as=jnp.bfloat16):
    entries = width * jax.random.normal(stream_key, extent, jnp.float32)
    if pieces:
        entries = entries * levels(stream_key, extent, pieces, -0.22, 0.18)
    return jnp.clip(with_spikes(entries, jax.random.fold_in(stream_key, 3), *heavy), -bound, bound).astype(held_as)


def setup_inputs(seed: int = 0, part: int = 0) -> dict:
    seeds = jax.random.split(jax.random.key(seed), 4)
    part_keys = jax.random.split(jax.random.fold_in(seeds[3], part), 4)
    return {
        "train_down": bell_draw_with(part_keys[0], (EXPERTS, D_EXPERT, D_MODEL), D_EXPERT ** -0.5, 0.25, ((0, 4), (2, 16)), (2, 1, 16, 2.0), jnp.float32),
        "router_weight": gaussian(part_keys[1], (D_MODEL, EXPERTS), D_MODEL ** -0.5, 0.125, ((0, 16), (1, 4)), jnp.float32),
        "router_gain": jnp.clip(1.0 + 0.15 * jax.random.normal(part_keys[2], (D_MODEL,), jnp.float32), 0.25, 1.75),
    }


def reference(train_down, router_weight, router_gain):
    scale_down = jnp.max(jnp.abs(train_down), axis=2)
    ready_down = (train_down / jnp.expand_dims(scale_down, 2)).astype(jnp.bfloat16)
    serve_router = (router_weight * router_gain[:, None]).astype(jnp.bfloat16)
    return ready_down, scale_down, serve_router
```

```python
import functools

import jax
import jax.numpy as jnp
from jax import lax
from jax.experimental import pallas as pl
from jax.experimental.pallas import tpu as pltpu
from jax.sharding import PartitionSpec as P

MESH = pl.DeviceIdType.MESH
LANES = 128
EARLY = 2
GROUP = 2

PEERS = [(d, c) for d in (4, 3, 5, 2, 6, 1, 7) for c in (0, 1)] + [(0, 1)]


def exchange_kernel(
    units,
    x_ref, w_ref, g_ref,
    ready_ref, scale_ref, router_ref,
    xv, sent, early, early_in, early_scale, peaks, peaks_in, scales,
    x_sem, send_sem, recv_sem, small_send, small_recv, cross_send, cross_recv,
):
    chips, banks = units
    experts, rows, _ = x_ref.shape
    per = ready_ref.shape[1]
    me = lax.axis_index("zero")
    chip, core = me // 2, lax.rem(me, 2)
    bank = lax.axis_index("bank")
    mine = pl.ds(pl.multiple_of(me * LANES, LANES), LANES)

    def peer(k):
        ahead, other = PEERS[k]
        chip_to = lax.rem(chip + ahead, chips)
        core_to = lax.rem(core + other, 2)
        return chip_to, core_to, chip_to * 2 + core_to

    def load(e):
        return pltpu.make_async_copy(x_ref.at[e], xv.at[e], x_sem.at[e])

    for e in range(experts):
        load(e).start()

    barrier = pltpu.get_barrier_semaphore()
    for k in range(len(PEERS)):
        pl.semaphore_signal(barrier, inc=1, device_id={"zero": peer(k)[2]}, device_id_type=MESH)
    for b in range(1, banks):
        to = lax.rem(bank + b, banks)
        pl.semaphore_signal(barrier, inc=1, device_id={"bank": to}, device_id_type=MESH)

    rank = pl.ds(pl.multiple_of(bank * 16, 16), 16)
    router_ref[rank, mine] = (w_ref[...] * g_ref[...]).astype(jnp.bfloat16)

    def peak(e, block):
        tile = jnp.abs(xv[e, pl.ds(block * LANES, LANES), :])
        return jnp.max(tile.T, axis=0, keepdims=True)

    for e in range(EARLY):
        load(e).wait()
        early[e] = jnp.concatenate([peak(e, b) for b in range(chips)], axis=0)

    pl.semaphore_wait(barrier, len(PEERS) + banks - 1)

    def copy(src, dst, kind, k, to):
        return pltpu.make_async_remote_copy(
            src_ref=src, dst_ref=dst,
            send_sem=small_send.at[kind, k], recv_sem=small_recv.at[kind, k],
            device_id=to, device_id_type=MESH,
        )

    def early_copy(k):
        return copy(early, early_in.at[k], 0, k, {"zero": peer(k)[2]})

    def peaks_copy(k):
        chip_to, core_to, to = peer(k)
        tile = pl.ds(pl.multiple_of(core_to * 8, 8), 8)
        return copy(peaks.at[chip_to, tile], peaks_in.at[k], 1, k, {"zero": to})

    own = pl.ds(pl.multiple_of(core * 8, 8), 8)

    def scales_copy(k):
        return copy(scales.at[chip, own], scales.at[chip, own], 2, k, {"zero": peer(k)[2]})

    def router_copy(k):
        return copy(router_ref.at[rank, mine], router_ref.at[rank, mine], 3, k, {"zero": peer(k)[2]})

    def cross_copy(b):
        to = lax.rem(bank + b, banks)
        return pltpu.make_async_remote_copy(
            src_ref=router_ref.at[rank], dst_ref=router_ref.at[rank],
            send_sem=cross_send.at[b - 1], recv_sem=cross_recv.at[b - 1],
            device_id={"bank": to}, device_id_type=MESH,
        )

    def block_copy(group, e0, n, k):
        to = peer(k)[2]
        return pltpu.make_async_remote_copy(
            src_ref=sent.at[to, pl.ds(e0, n)],
            dst_ref=ready_ref.at[pl.ds(e0, n), :, mine],
            send_sem=send_sem.at[group, k], recv_sem=recv_sem.at[group, k],
            device_id={"zero": to}, device_id_type=MESH,
        )

    every = range(len(PEERS))
    for k in every:
        early_copy(k).start()

    for e in range(EARLY, 8):
        load(e).wait()

    def peak_rows(block, e0):
        rows_of = [
            early[e0 + i, pl.ds(block, 1), :] if e0 + i < EARLY else peak(e0 + i, block)
            for i in range(8)
        ]
        peaks[block, pl.ds(e0, 8), :] = jnp.concatenate(rows_of, axis=0)

    pl.loop(0, chips)(lambda block: peak_rows(block, 0))
    for e in range(8, experts):
        load(e).wait()
    pl.loop(0, chips)(lambda block: peak_rows(block, 8))

    for k in every:
        peaks_copy(k).start()
    for k in every:
        router_copy(k).start()

    def scaled(e, row_of):
        for b in range(chips):
            inverse = 1.0 / row_of(b)
            column = jnp.broadcast_to(inverse, (LANES, LANES)).T
            y = (xv[e, pl.ds(b * LANES, LANES), :] * column).astype(jnp.bfloat16)
            sent[2 * b, e] = y[:per]
            sent[2 * b + 1, e] = y[per:]
        ready_ref[e, :, mine] = sent[me, e]

    for k in every:
        early_copy(k).wait_recv()
    top = early[...]
    for k in every:
        top = jnp.maximum(top, early_in[k])
    early_scale[...] = top
    for e in range(EARLY):
        scaled(e, lambda b: early_scale[e, b : b + 1, :])
        if e == 0:
            for k in every:
                block_copy(0, 0, 1, k).start()

    for k in every:
        peaks_copy(k).wait_recv()
    top = peaks[chip, own, :]
    for k in every:
        top = jnp.maximum(top, peaks_in[k])
    scales[chip, own, :] = top
    for k in every:
        scales_copy(k).start()
    for k in every:
        block_copy(1, 1, EARLY - 1, k).start()

    for k in every:
        router_copy(k).wait_recv()
    for b in range(1, banks):
        cross_copy(b).start()

    for k in every:
        scales_copy(k).wait_recv()
    whole = scales[chip]
    scale_ref[...] = jnp.where(core == 0, whole[:, :per], whole[:, per:])

    groups = (experts - EARLY) // GROUP

    @pl.loop(0, groups)
    def _(i):
        e0 = EARLY + i * GROUP
        for j in range(GROUP):
            e = e0 + j
            scaled(e, lambda b: scales[b, pl.ds(e, 1), :])
        for k in every:
            block_copy(2 + i, e0, GROUP, k).start()

    for k in every:
        early_copy(k).wait_send()
        peaks_copy(k).wait_send()
        scales_copy(k).wait_send()
        router_copy(k).wait_send()
    for b in range(1, banks):
        cross_copy(b).wait()
    for k in every:
        block_copy(0, 0, 1, k).wait()
        block_copy(1, 1, EARLY - 1, k).wait()

    @pl.loop(0, groups)
    def _(i):
        for k in every:
            block_copy(2 + i, EARLY + i * GROUP, GROUP, k).wait()


def solution(mesh):
    chips, banks = mesh.shape["zero"] // 2, mesh.shape["bank"]

    def per_device(train_down, router_weight, router_gain):
        experts, rows, lanes = train_down.shape
        per = rows // (2 * chips)
        columns = router_weight.shape[1]
        vmem = pl.BlockSpec(memory_space=pltpu.VMEM)
        groups = 2 + (experts - EARLY) // GROUP
        n = len(PEERS)
        ready, scale, router = pl.pallas_call(
            functools.partial(exchange_kernel, (chips, banks)),
            out_shape=(
                jax.ShapeDtypeStruct((experts, per, 2 * chips * lanes), jnp.bfloat16),
                jax.ShapeDtypeStruct((experts, per), jnp.float32),
                jax.ShapeDtypeStruct((columns * banks, 2 * chips * LANES), jnp.bfloat16),
            ),
            in_specs=[pl.BlockSpec(memory_space=pltpu.HBM), vmem, vmem],
            out_specs=(vmem, vmem, vmem),
            scratch_shapes=[
                pltpu.VMEM((experts, rows, lanes), jnp.float32),
                pltpu.VMEM((2 * chips, experts, per, lanes), jnp.bfloat16),
                pltpu.VMEM((EARLY, chips, LANES), jnp.float32),
                pltpu.VMEM((n, EARLY, chips, LANES), jnp.float32),
                pltpu.VMEM((EARLY, chips, LANES), jnp.float32),
                pltpu.VMEM((chips, experts, LANES), jnp.float32),
                pltpu.VMEM((n, 8, LANES), jnp.float32),
                pltpu.VMEM((chips, experts, LANES), jnp.float32),
                pltpu.SemaphoreType.DMA((experts,)),
                pltpu.SemaphoreType.DMA((groups, n)),
                pltpu.SemaphoreType.DMA((groups, n)),
                pltpu.SemaphoreType.DMA((4, n)),
                pltpu.SemaphoreType.DMA((4, n)),
                pltpu.SemaphoreType.DMA((banks - 1,)),
                pltpu.SemaphoreType.DMA((banks - 1,)),
            ],
            compiler_params=pltpu.CompilerParams(
                collective_id=0, has_side_effects=True, vmem_limit_bytes=40 * 2**20
            ),
            name="exchange",
        )(train_down, router_weight.T, router_gain.reshape(1, -1))
        return ready, scale, router.T

    return jax.shard_map(
        per_device,
        mesh=mesh,
        in_specs=(P(("unit", "bank"), None, "zero"), P(("unit", "zero"), "bank"), P(("unit", "zero"))),
        out_specs=(P(("unit", "bank"), "zero", None), P(("unit", "bank"), "zero"), P("unit", None)),
        check_vma=False,
    )
```

```python
import functools

import jax
import jax.numpy as jnp
from jax import lax
from jax.experimental import pallas as pl
from jax.experimental.pallas import tpu as pltpu
from jax.sharding import PartitionSpec as P

MESH = pl.DeviceIdType.MESH
LANES = 128
HALF = 8
EARLY = 2
GROUP = 2
STORES = 8

PEERS = [(d, c) for d in (4, 3, 5, 2, 6, 1, 7) for c in (0, 1)] + [(0, 1)]
ALIKE = [k for k, (d, c) in enumerate(PEERS) if c == 0]
PARTNER = len(PEERS) - 1
PEAKS, SCALES, ROUTER, FORWARD = 1, 2, 3, 4


def exchange_kernel(
    units,
    x_ref, w_ref, g_ref,
    ready_ref, scale_ref, router_ref,
    xv, wv, gv, sent, early, early_in, early_scale,
    peaks, pair_in, merged, peaks_in, scales, tiles,
    x_sem, send_sem, recv_sem, small_send, small_recv, cross_send, cross_recv,
):
    chips, banks = units
    experts, rows, _ = x_ref.shape
    per = ready_ref.shape[1]
    me = lax.axis_index("zero")
    chip, core = me // 2, lax.rem(me, 2)
    bank = lax.axis_index("bank")
    mine = pl.ds(pl.multiple_of(me * LANES, LANES), LANES)
    every = range(len(PEERS))

    def peer(k):
        ahead, other = PEERS[k]
        chip_to = lax.rem(chip + ahead, chips)
        core_to = lax.rem(core + other, 2)
        return chip_to, {"zero": chip_to * 2 + core_to}

    def load(e):
        return pltpu.make_async_copy(x_ref.at[e], xv.at[e], x_sem.at[e])

    for e in range(experts):
        load(e).start()
    weight_in = pltpu.make_async_copy(w_ref, wv, x_sem.at[experts])
    gain_in = pltpu.make_async_copy(g_ref, gv, x_sem.at[experts + 1])
    weight_in.start()
    gain_in.start()

    barrier = pltpu.get_barrier_semaphore()
    for k in every:
        pl.semaphore_signal(barrier, inc=1, device_id=peer(k)[1], device_id_type=MESH)
    for b in range(1, banks):
        to = lax.rem(bank + b, banks)
        pl.semaphore_signal(barrier, inc=1, device_id={"bank": to}, device_id_type=MESH)

    def peak(e, block):
        tile = jnp.abs(xv[e, pl.ds(block * LANES, LANES), :])
        return jnp.max(tile.T, axis=0, keepdims=True)

    for e in range(EARLY):
        load(e).wait()
        early[e] = jnp.concatenate([peak(e, b) for b in range(chips)], axis=0)

    def copy(src, dst, kind, k):
        return pltpu.make_async_remote_copy(
            src_ref=src, dst_ref=dst,
            send_sem=small_send.at[kind, k], recv_sem=small_recv.at[kind, k],
            device_id=peer(k)[1], device_id_type=MESH,
        )

    def early_copy(k):
        return copy(early, early_in.at[k], 0, k)

    def peaks_copy(k):
        return copy(merged.at[peer(k)[0]], peaks_in.at[k], PEAKS, k)

    pair_copy = copy(peaks.at[1 - core], pair_in, PEAKS, PARTNER)

    def scales_copy(k):
        place = scales.at[core, chip]
        return copy(place, place, SCALES, k)

    scales_pass = copy(scales.at[core], scales.at[core], SCALES, PARTNER)
    rank = pl.ds(pl.multiple_of(bank * 16, 16), 16)
    column = pl.ds(pl.multiple_of(chip * LANES, LANES), LANES)

    def router_copy(k):
        place = tiles.at[core, rank, column]
        return copy(place, place, ROUTER, k)

    def cross_copy(b):
        place = tiles.at[core, rank]
        return pltpu.make_async_remote_copy(
            src_ref=place, dst_ref=place,
            send_sem=cross_send.at[b - 1], recv_sem=cross_recv.at[b - 1],
            device_id={"bank": lax.rem(bank + b, banks)}, device_id_type=MESH,
        )

    router_pass = copy(tiles.at[core], tiles.at[core], ROUTER, PARTNER)

    def block_copy(group, e0, n, k):
        chip_to, to = peer(k)
        return pltpu.make_async_remote_copy(
            src_ref=sent.at[to["zero"], pl.ds(e0, n)],
            dst_ref=ready_ref.at[pl.ds(e0, n), :, mine],
            send_sem=send_sem.at[group, k], recv_sem=recv_sem.at[group, k],
            device_id=to, device_id_type=MESH,
        )

    pl.semaphore_wait(barrier, len(PEERS) + banks - 1)
    for k in every:
        early_copy(k).start()
    for e in range(EARLY, experts):
        load(e).wait()

    def half_peaks(half):
        @pl.loop(0, chips)
        def _(block):
            found = [peak(half * HALF + i, block) for i in range(HALF)]
            peaks[half, block] = jnp.concatenate(found, axis=0)

    half_peaks(1 - core)
    pair_copy.start()
    half_peaks(core)
    pair_copy.wait_recv()
    merged[...] = jnp.maximum(peaks[core], pair_in[...])
    for k in ALIKE:
        peaks_copy(k).start()
    weight_in.wait()
    gain_in.wait()
    tiles[core, rank, column] = (wv[...] * gv[...]).astype(jnp.bfloat16)
    for k in ALIKE:
        router_copy(k).start()

    def scaled(e, row_of):
        for b in range(chips):
            inverse = 1.0 / row_of(b)
            spread = jnp.broadcast_to(inverse, (LANES, LANES)).T
            y = (xv[e, pl.ds(b * LANES, LANES), :] * spread).astype(jnp.bfloat16)
            sent[2 * b, e] = y[:per]
            sent[2 * b + 1, e] = y[per:]
        ready_ref[e, :, mine] = sent[me, e]

    for k in every:
        early_copy(k).wait_recv()
    top = early[...]
    for k in every:
        top = jnp.maximum(top, early_in[k])
    early_scale[...] = top
    for e in range(EARLY):
        scaled(e, lambda b: early_scale[e, b : b + 1, :])
        if e == 0:
            for k in every:
                block_copy(0, 0, 1, k).start()
    for k in ALIKE:
        peaks_copy(k).wait_recv()
    top = merged[chip]
    for k in ALIKE:
        top = jnp.maximum(top, peaks_in[k])
    scales[core, chip] = top
    for k in ALIKE:
        scales_copy(k).start()
    for k in every:
        block_copy(1, 1, EARLY - 1, k).start()
    for k in ALIKE:
        router_copy(k).wait_recv()
    for b in range(1, banks):
        cross_copy(b).start()
    for k in ALIKE:
        scales_copy(k).wait_recv()
    scales_pass.start()
    scales_pass.wait_recv()
    groups = (experts - EARLY) // GROUP

    @pl.loop(0, groups)
    def _(i):
        e0 = EARLY + i * GROUP
        for j in range(GROUP):
            e = e0 + j
            scaled(e, lambda b: scales[e // HALF, b, pl.ds(lax.rem(e, HALF), 1), :])
        for k in every:
            block_copy(2 + i, e0, GROUP, k).start()

    whole = jnp.concatenate([scales[0, chip], scales[1, chip]], axis=0)
    scale_ref[...] = jnp.where(core == 0, whole[:, :per], whole[:, per:])
    for b in range(1, banks):
        cross_copy(b).wait()
    router_pass.start()
    router_pass.wait()
    for j in range(chips):
        for c in range(2):
            at = (2 * j + c) * LANES
            router_ref[:, at : at + LANES] = tiles[c, :, j * LANES : (j + 1) * LANES]
    for k in every:
        early_copy(k).wait_send()
    for k in ALIKE:
        peaks_copy(k).wait_send()
        scales_copy(k).wait_send()
        router_copy(k).wait_send()
    pair_copy.wait_send()
    scales_pass.wait_send()
    for k in every:
        block_copy(0, 0, 1, k).wait()
        block_copy(1, 1, EARLY - 1, k).wait()

    @pl.loop(0, groups)
    def _(i):
        for k in every:
            block_copy(2 + i, EARLY + i * GROUP, GROUP, k).wait()


def store_kernel(ready, scale, router, ready_ref, scale_ref, router_ref, sem):
    step = ready.shape[0] // STORES
    parts = [pl.ds(i * step, step) for i in range(STORES)]
    moves = [(ready.at[p], ready_ref.at[p]) for p in parts]
    moves += [(scale, scale_ref), (router, router_ref)]
    copies = [pltpu.make_async_copy(*m, sem.at[i]) for i, m in enumerate(moves)]
    for c in copies:
        c.start()
    for c in copies:
        c.wait()


def solution(mesh):
    chips, banks = mesh.shape["zero"] // 2, mesh.shape["bank"]

    def per_device(train_down, router_weight, router_gain):
        experts, rows, lanes = train_down.shape
        per = rows // (2 * chips)
        columns = router_weight.shape[1]
        vmem = pl.BlockSpec(memory_space=pltpu.VMEM)
        hbm = pl.BlockSpec(memory_space=pltpu.HBM)
        groups = 2 + (experts - EARLY) // GROUP
        n = len(PEERS)
        outs = (
            jax.ShapeDtypeStruct((experts, per, 2 * chips * lanes), jnp.bfloat16),
            jax.ShapeDtypeStruct((experts, per), jnp.float32),
            jax.ShapeDtypeStruct((columns * banks, 2 * chips * LANES), jnp.bfloat16),
        )
        held = [
            pltpu.with_memory_space_constraint(a, pltpu.HBM)
            for a in (train_down, router_weight.T, router_gain.reshape(1, -1))
        ]
        made = pl.pallas_call(
            functools.partial(exchange_kernel, (chips, banks)),
            out_shape=outs,
            in_specs=[hbm, hbm, hbm],
            out_specs=(vmem, vmem, vmem),
            scratch_shapes=[
                pltpu.VMEM((experts, rows, lanes), jnp.float32),
                pltpu.VMEM((columns, LANES), jnp.float32),
                pltpu.VMEM((1, LANES), jnp.float32),
                pltpu.VMEM((2 * chips, experts, per, lanes), jnp.bfloat16),
                pltpu.VMEM((EARLY, chips, LANES), jnp.float32),
                pltpu.VMEM((n, EARLY, chips, LANES), jnp.float32),
                pltpu.VMEM((EARLY, chips, LANES), jnp.float32),
                pltpu.VMEM((2, chips, HALF, LANES), jnp.float32),
                pltpu.VMEM((chips, HALF, LANES), jnp.float32),
                pltpu.VMEM((chips, HALF, LANES), jnp.float32),
                pltpu.VMEM((n, HALF, LANES), jnp.float32),
                pltpu.VMEM((2, chips, HALF, LANES), jnp.float32),
                pltpu.VMEM((2, columns * banks, chips * LANES), jnp.bfloat16),
                pltpu.SemaphoreType.DMA((experts + 2,)),
                pltpu.SemaphoreType.DMA((groups, n)),
                pltpu.SemaphoreType.DMA((groups, n)),
                pltpu.SemaphoreType.DMA((4, n)),
                pltpu.SemaphoreType.DMA((4, n)),
                pltpu.SemaphoreType.DMA((banks - 1,)),
                pltpu.SemaphoreType.DMA((banks - 1,)),
            ],
            compiler_params=pltpu.CompilerParams(
                collective_id=0, has_side_effects=True, vmem_limit_bytes=24 * 2**20
            ),
            name="exchange",
        )(*held)
        ready, scale, router = pl.pallas_call(
            store_kernel,
            out_shape=outs,
            in_specs=[vmem, vmem, vmem],
            out_specs=(hbm, hbm, hbm),
            scratch_shapes=[pltpu.SemaphoreType.DMA((STORES + 2,))],
            compiler_params=pltpu.CompilerParams(vmem_limit_bytes=4 * 2**20),
            name="store",
        )(*(pltpu.with_memory_space_constraint(a, pltpu.VMEM) for a in made))
        return ready, scale, router.T

    return jax.shard_map(
        per_device,
        mesh=mesh,
        in_specs=(P(("unit", "bank"), None, "zero"), P(("unit", "zero"), "bank"), P(("unit", "zero"))),
        out_specs=(P(("unit", "bank"), "zero", None), P(("unit", "bank"), "zero"), P("unit", None)),
        check_vma=False,
    )
```

```python
import functools

import jax
import jax.numpy as jnp
from jax import lax
from jax.experimental import pallas as pl
from jax.experimental.pallas import tpu as pltpu
from jax.sharding import PartitionSpec as P

MESH = pl.DeviceIdType.MESH
LANES = 128
HALF = 8
EARLY = 2
GROUP = 2
STORES = 8

PEERS = [(d, c) for d in (4, 3, 5, 2, 6, 1, 7) for c in (0, 1)] + [(0, 1)]
ALIKE = [k for k, (d, c) in enumerate(PEERS) if c == 0]
PARTNER = len(PEERS) - 1
FIRST, PEAKS, SCALES, ROUTER, PAIR, PASS, SIDE, WHOLE, BLOCKS = range(9)


def exchange_kernel(
    units,
    x_ref, w_ref, g_ref,
    ready_ref, scale_ref, router_ref,
    xv, wv, gv, sent, early, early_in, early_scale,
    peaks, pair_in, merged, peaks_in, scales, tiles,
    x_sem, send_sem, recv_sem,
):
    chips, banks = units
    experts, rows, _ = x_ref.shape
    per = ready_ref.shape[1]
    me = lax.axis_index("zero")
    chip, core = me // 2, lax.rem(me, 2)
    bank = lax.axis_index("bank")
    mine = pl.ds(pl.multiple_of(me * LANES, LANES), LANES)
    every = range(len(PEERS))

    def peer(k):
        ahead, other = PEERS[k]
        chip_to = lax.rem(chip + ahead, chips)
        core_to = lax.rem(core + other, 2)
        return chip_to, {"zero": chip_to * 2 + core_to}

    def load(e):
        return pltpu.make_async_copy(x_ref.at[e], xv.at[e], x_sem.at[e])

    for e in range(experts):
        load(e).start()
    weight_in = pltpu.make_async_copy(w_ref, wv, x_sem.at[experts])
    gain_in = pltpu.make_async_copy(g_ref, gv, x_sem.at[experts + 1])
    weight_in.start()
    gain_in.start()

    barrier = pltpu.get_barrier_semaphore()
    for k in every:
        pl.semaphore_signal(barrier, inc=1, device_id=peer(k)[1], device_id_type=MESH)
    for b in range(1, banks):
        to = lax.rem(bank + b, banks)
        pl.semaphore_signal(barrier, inc=1, device_id={"bank": to}, device_id_type=MESH)

    def peak(e, block):
        tile = jnp.abs(xv[e, pl.ds(block * LANES, LANES), :])
        return jnp.max(tile.T, axis=0, keepdims=True)

    for e in range(EARLY):
        load(e).wait()
        early[e] = jnp.concatenate([peak(e, b) for b in range(chips)], axis=0)

    def copy(src, dst, kind, k, to=None):
        return pltpu.make_async_remote_copy(
            src_ref=src, dst_ref=dst,
            send_sem=send_sem.at[kind], recv_sem=recv_sem.at[kind],
            device_id=peer(k)[1] if to is None else to, device_id_type=MESH,
        )

    def await_all(ref, sem):
        pltpu.make_async_copy(ref, ref, sem).wait()

    def early_copy(k):
        return copy(early, early_in.at[k], FIRST, k)

    def peaks_copy(k):
        return copy(merged.at[peer(k)[0]], peaks_in.at[k // 2], PEAKS, k)

    pair_copy = copy(peaks.at[1 - core], pair_in, PAIR, PARTNER)

    def scales_copy(k):
        place = scales.at[core, chip]
        return copy(place, place, SCALES, k)

    scales_pass = copy(scales.at[core], scales.at[core], PASS, PARTNER)
    rank = pl.ds(pl.multiple_of(bank * 16, 16), 16)
    column = pl.ds(pl.multiple_of(chip * LANES, LANES), LANES)
    sevenths = tiles.at[0, pl.ds(0, 16), pl.ds(0, (chips - 1) * LANES)]

    def router_copy(k):
        place = tiles.at[core, rank, column]
        return copy(place, place, ROUTER, k)

    def cross_copy(b):
        place = tiles.at[core, rank]
        return copy(place, place, SIDE, None, {"bank": lax.rem(bank + b, banks)})

    router_pass = copy(tiles.at[core], tiles.at[core], WHOLE, PARTNER)

    def block_copy(e0, n, k):
        to = peer(k)[1]
        experts_of = pl.ds(e0, n)
        return copy(sent.at[to["zero"], experts_of], ready_ref.at[experts_of, :, mine], BLOCKS, k)

    pl.semaphore_wait(barrier, len(PEERS) + banks - 1)
    for k in every:
        early_copy(k).start()
    for e in range(EARLY, experts):
        load(e).wait()

    def half_peaks(half):
        @pl.loop(0, chips)
        def _(block):
            found = [peak(half * HALF + i, block) for i in range(HALF)]
            peaks[half, block] = jnp.concatenate(found, axis=0)

    half_peaks(1 - core)
    pair_copy.start()
    half_peaks(core)
    pair_copy.wait_recv()
    merged[...] = jnp.maximum(peaks[core], pair_in[...])
    for k in ALIKE:
        peaks_copy(k).start()
    weight_in.wait()
    gain_in.wait()
    tiles[core, rank, column] = (wv[...] * gv[...]).astype(jnp.bfloat16)
    for k in ALIKE:
        router_copy(k).start()

    def scaled(e, row_of):
        for b in range(chips):
            inverse = 1.0 / row_of(b)
            spread = jnp.broadcast_to(inverse, (LANES, LANES)).T
            y = (xv[e, pl.ds(b * LANES, LANES), :] * spread).astype(jnp.bfloat16)
            sent[2 * b, e] = y[:per]
            sent[2 * b + 1, e] = y[per:]
        ready_ref[e, :, mine] = sent[me, e]

    await_all(early_in, recv_sem.at[FIRST])
    top = early[...]
    for k in every:
        top = jnp.maximum(top, early_in[k])
    early_scale[...] = top
    for e in range(EARLY):
        scaled(e, lambda b: early_scale[e, b : b + 1, :])
        if e == 0:
            for k in every:
                block_copy(0, 1, k).start()
    await_all(peaks_in, recv_sem.at[PEAKS])
    top = merged[chip]
    for k in ALIKE:
        top = jnp.maximum(top, peaks_in[k // 2])
    scales[core, chip] = top
    for k in ALIKE:
        scales_copy(k).start()
    for k in every:
        block_copy(1, EARLY - 1, k).start()
    await_all(sevenths, recv_sem.at[ROUTER])
    for b in range(1, banks):
        cross_copy(b).start()
    await_all(peaks_in, recv_sem.at[SCALES])
    scales_pass.start()
    scales_pass.wait_recv()
    groups = (experts - EARLY) // GROUP

    @pl.loop(0, groups)
    def _(i):
        e0 = EARLY + i * GROUP
        for j in range(GROUP):
            e = e0 + j
            scaled(e, lambda b: scales[e // HALF, b, pl.ds(lax.rem(e, HALF), 1), :])
        for k in every:
            block_copy(e0, GROUP, k).start()

    whole = jnp.concatenate([scales[0, chip], scales[1, chip]], axis=0)
    scale_ref[...] = jnp.where(core == 0, whole[:, :per], whole[:, per:])
    await_all(tiles.at[core, pl.ds(0, 16 * (banks - 1))], recv_sem.at[SIDE])
    router_pass.start()
    router_pass.wait()
    for j in range(chips):
        for c in range(2):
            at = (2 * j + c) * LANES
            router_ref[:, at : at + LANES] = tiles[c, :, j * LANES : (j + 1) * LANES]
    await_all(early_in, send_sem.at[FIRST])
    await_all(peaks_in, send_sem.at[PEAKS])
    await_all(peaks_in, send_sem.at[SCALES])
    await_all(sevenths, send_sem.at[ROUTER])
    await_all(tiles.at[core, pl.ds(0, 16 * (banks - 1))], send_sem.at[SIDE])
    pair_copy.wait_send()
    scales_pass.wait_send()
    blocks = sent.at[pl.ds(0, len(PEERS))]
    await_all(blocks, send_sem.at[BLOCKS])
    await_all(blocks, recv_sem.at[BLOCKS])


def store_kernel(ready, scale, router, ready_ref, scale_ref, router_ref, sem):
    step = ready.shape[0] // STORES
    parts = [pl.ds(i * step, step) for i in range(STORES)]
    moves = [(ready.at[p], ready_ref.at[p]) for p in parts]
    moves += [(scale, scale_ref), (router, router_ref)]
    copies = [pltpu.make_async_copy(*m, sem.at[i]) for i, m in enumerate(moves)]
    for c in copies:
        c.start()
    for c in copies:
        c.wait()


def solution(mesh):
    chips, banks = mesh.shape["zero"] // 2, mesh.shape["bank"]

    def per_device(train_down, router_weight, router_gain):
        experts, rows, lanes = train_down.shape
        per = rows // (2 * chips)
        columns = router_weight.shape[1]
        vmem = pl.BlockSpec(memory_space=pltpu.VMEM)
        hbm = pl.BlockSpec(memory_space=pltpu.HBM)
        n = len(PEERS)
        outs = (
            jax.ShapeDtypeStruct((experts, per, 2 * chips * lanes), jnp.bfloat16),
            jax.ShapeDtypeStruct((experts, per), jnp.float32),
            jax.ShapeDtypeStruct((columns * banks, 2 * chips * LANES), jnp.bfloat16),
        )
        held = [
            pltpu.with_memory_space_constraint(a, pltpu.HBM)
            for a in (train_down, router_weight.T, router_gain.reshape(1, -1))
        ]
        made = pl.pallas_call(
            functools.partial(exchange_kernel, (chips, banks)),
            out_shape=outs,
            in_specs=[hbm, hbm, hbm],
            out_specs=(vmem, vmem, vmem),
            scratch_shapes=[
                pltpu.VMEM((experts, rows, lanes), jnp.float32),
                pltpu.VMEM((columns, LANES), jnp.float32),
                pltpu.VMEM((1, LANES), jnp.float32),
                pltpu.VMEM((2 * chips, experts, per, lanes), jnp.bfloat16),
                pltpu.VMEM((EARLY, chips, LANES), jnp.float32),
                pltpu.VMEM((n, EARLY, chips, LANES), jnp.float32),
                pltpu.VMEM((EARLY, chips, LANES), jnp.float32),
                pltpu.VMEM((2, chips, HALF, LANES), jnp.float32),
                pltpu.VMEM((chips, HALF, LANES), jnp.float32),
                pltpu.VMEM((chips, HALF, LANES), jnp.float32),
                pltpu.VMEM((chips - 1, HALF, LANES), jnp.float32),
                pltpu.VMEM((2, chips, HALF, LANES), jnp.float32),
                pltpu.VMEM((2, columns * banks, chips * LANES), jnp.bfloat16),
                pltpu.SemaphoreType.DMA((experts + 2,)),
                pltpu.SemaphoreType.DMA((BLOCKS + 1,)),
                pltpu.SemaphoreType.DMA((BLOCKS + 1,)),
            ],
            compiler_params=pltpu.CompilerParams(
                collective_id=0, has_side_effects=True, vmem_limit_bytes=24 * 2**20
            ),
            name="exchange",
        )(*held)
        ready, scale, router = pl.pallas_call(
            store_kernel,
            out_shape=outs,
            in_specs=[vmem, vmem, vmem],
            out_specs=(hbm, hbm, hbm),
            scratch_shapes=[pltpu.SemaphoreType.DMA((STORES + 2,))],
            compiler_params=pltpu.CompilerParams(vmem_limit_bytes=4 * 2**20),
            name="store",
        )(*(pltpu.with_memory_space_constraint(a, pltpu.VMEM) for a in made))
        return ready, scale, router.T

    return jax.shard_map(
        per_device,
        mesh=mesh,
        in_specs=(P(("unit", "bank"), None, "zero"), P(("unit", "zero"), "bank"), P(("unit", "zero"))),
        out_specs=(P(("unit", "bank"), "zero", None), P(("unit", "bank"), "zero"), P("unit", None)),
        check_vma=False,
    )
```

```python
import functools

import jax
import jax.numpy as jnp
from jax import lax
from jax.experimental import pallas as pl
from jax.experimental.pallas import tpu as pltpu
from jax.sharding import PartitionSpec as P

MESH = pl.DeviceIdType.MESH
LANES = 128
HALF = 8
EARLY = 2
GROUP = 2
STORES = 8

PEERS = [(d, c) for c in (1, 0) for d in (4, 3, 5, 2, 6, 1, 7)] + [(0, 1)]
ALIKE = [k for k, (d, c) in enumerate(PEERS) if c == 0]
PARTNER = len(PEERS) - 1
FIRST, PEAKS, SCALES, ROUTER, PAIR, PASS, SIDE, WHOLE, BLOCKS = range(9)


def exchange_kernel(
    units,
    x_ref, w_ref, g_ref,
    ready_ref, scale_ref, router_ref,
    xv, wv, gv, sent, early, early_in, early_scale,
    peaks, pair_in, merged, peaks_in, scales, tiles,
    x_sem, send_sem, recv_sem,
):
    chips, banks = units
    experts, rows, _ = x_ref.shape
    per = ready_ref.shape[1]
    me = lax.axis_index("zero")
    chip, core = me // 2, lax.rem(me, 2)
    bank = lax.axis_index("bank")
    mine = pl.ds(pl.multiple_of(me * LANES, LANES), LANES)
    every = range(len(PEERS))

    def peer(k):
        ahead, other = PEERS[k]
        chip_to = lax.rem(chip + ahead, chips)
        core_to = lax.rem(core + other, 2)
        return chip_to, {"zero": chip_to * 2 + core_to}

    def load(e):
        return pltpu.make_async_copy(x_ref.at[e], xv.at[e], x_sem.at[e])

    for e in range(experts):
        load(e).start()
    weight_in = pltpu.make_async_copy(w_ref, wv, x_sem.at[experts])
    gain_in = pltpu.make_async_copy(g_ref, gv, x_sem.at[experts + 1])
    weight_in.start()
    gain_in.start()

    barrier = pltpu.get_barrier_semaphore()
    for k in every:
        pl.semaphore_signal(barrier, inc=1, device_id=peer(k)[1], device_id_type=MESH)
    for b in range(1, banks):
        to = lax.rem(bank + b, banks)
        pl.semaphore_signal(barrier, inc=1, device_id={"bank": to}, device_id_type=MESH)

    def peak(e, block):
        tile = jnp.abs(xv[e, pl.ds(block * LANES, LANES), :])
        return jnp.max(tile.T, axis=0, keepdims=True)

    for e in range(EARLY):
        load(e).wait()
        early[e] = jnp.concatenate([peak(e, b) for b in range(chips)], axis=0)

    def copy(src, dst, kind, k, to=None):
        return pltpu.make_async_remote_copy(
            src_ref=src, dst_ref=dst,
            send_sem=send_sem.at[kind], recv_sem=recv_sem.at[kind],
            device_id=peer(k)[1] if to is None else to, device_id_type=MESH,
        )

    def await_all(ref, sem):
        pltpu.make_async_copy(ref, ref, sem).wait()

    def early_copy(k):
        return copy(early, early_in.at[k], FIRST, k)

    def peaks_copy(k):
        return copy(merged.at[peer(k)[0]], peaks_in.at[ALIKE.index(k)], PEAKS, k)

    pair_copy = copy(peaks.at[1 - core], pair_in, PAIR, PARTNER)

    def scales_copy(k):
        place = scales.at[core, chip]
        return copy(place, place, SCALES, k)

    scales_pass = copy(scales.at[core], scales.at[core], PASS, PARTNER)
    rank = pl.ds(pl.multiple_of(bank * 16, 16), 16)
    column = pl.ds(pl.multiple_of(chip * LANES, LANES), LANES)
    sevenths = tiles.at[0, pl.ds(0, 16), pl.ds(0, (chips - 1) * LANES)]

    def router_copy(k):
        place = tiles.at[core, rank, column]
        return copy(place, place, ROUTER, k)

    def cross_copy(b):
        place = tiles.at[core, rank]
        return copy(place, place, SIDE, None, {"bank": lax.rem(bank + b, banks)})

    router_pass = copy(tiles.at[core], tiles.at[core], WHOLE, PARTNER)

    def block_copy(e0, n, k):
        to = peer(k)[1]
        experts_of = pl.ds(e0, n)
        return copy(sent.at[to["zero"], experts_of], ready_ref.at[experts_of, :, mine], BLOCKS, k)

    pl.semaphore_wait(barrier, len(PEERS) + banks - 1)
    for k in every:
        early_copy(k).start()
    for e in range(EARLY, experts):
        load(e).wait()

    def half_peaks(half):
        @pl.loop(0, chips)
        def _(block):
            found = [peak(half * HALF + i, block) for i in range(HALF)]
            peaks[half, block] = jnp.concatenate(found, axis=0)

    half_peaks(1 - core)
    pair_copy.start()
    half_peaks(core)
    pair_copy.wait_recv()
    merged[...] = jnp.maximum(peaks[core], pair_in[...])
    for k in ALIKE:
        peaks_copy(k).start()
    weight_in.wait()
    gain_in.wait()
    tiles[core, rank, column] = (wv[...] * gv[...]).astype(jnp.bfloat16)
    for k in ALIKE:
        router_copy(k).start()

    def scaled(e, row_of):
        for b in range(chips):
            inverse = 1.0 / row_of(b)
            spread = jnp.broadcast_to(inverse, (LANES, LANES)).T
            y = (xv[e, pl.ds(b * LANES, LANES), :] * spread).astype(jnp.bfloat16)
            sent[2 * b, e] = y[:per]
            sent[2 * b + 1, e] = y[per:]
        ready_ref[e, :, mine] = sent[me, e]

    await_all(early_in, recv_sem.at[FIRST])
    top = early[...]
    for k in every:
        top = jnp.maximum(top, early_in[k])
    early_scale[...] = top
    for e in range(EARLY):
        scaled(e, lambda b: early_scale[e, b : b + 1, :])
        if e == 0:
            for k in every[:7]:
                block_copy(0, 1, k).start()
    await_all(peaks_in, recv_sem.at[PEAKS])
    top = merged[chip]
    for k in ALIKE:
        top = jnp.maximum(top, peaks_in[ALIKE.index(k)])
    scales[core, chip] = top
    for k in ALIKE:
        scales_copy(k).start()
    for k in every[7:]:
        block_copy(0, 1, k).start()
    for k in every:
        block_copy(1, EARLY - 1, k).start()
    await_all(sevenths, recv_sem.at[ROUTER])
    for b in range(1, banks):
        cross_copy(b).start()
    await_all(peaks_in, recv_sem.at[SCALES])
    scales_pass.start()
    scales_pass.wait_recv()
    groups = (experts - EARLY) // GROUP

    @pl.loop(0, groups)
    def _(i):
        e0 = EARLY + i * GROUP
        for j in range(GROUP):
            e = e0 + j
            scaled(e, lambda b: scales[e // HALF, b, pl.ds(lax.rem(e, HALF), 1), :])
        for k in every:
            block_copy(e0, GROUP, k).start()

    whole = jnp.concatenate([scales[0, chip], scales[1, chip]], axis=0)
    scale_ref[...] = jnp.where(core == 0, whole[:, :per], whole[:, per:])
    await_all(tiles.at[core, pl.ds(0, 16 * (banks - 1))], recv_sem.at[SIDE])
    router_pass.start()
    router_pass.wait()
    for j in range(chips):
        for c in range(2):
            at = (2 * j + c) * LANES
            router_ref[:, at : at + LANES] = tiles[c, :, j * LANES : (j + 1) * LANES]
    await_all(early_in, send_sem.at[FIRST])
    await_all(peaks_in, send_sem.at[PEAKS])
    await_all(peaks_in, send_sem.at[SCALES])
    await_all(sevenths, send_sem.at[ROUTER])
    await_all(tiles.at[core, pl.ds(0, 16 * (banks - 1))], send_sem.at[SIDE])
    pair_copy.wait_send()
    scales_pass.wait_send()
    blocks = sent.at[pl.ds(0, len(PEERS))]
    await_all(blocks, send_sem.at[BLOCKS])
    await_all(blocks, recv_sem.at[BLOCKS])


def store_kernel(ready, scale, router, ready_ref, scale_ref, router_ref, sem):
    step = ready.shape[0] // STORES
    parts = [pl.ds(i * step, step) for i in range(STORES)]
    moves = [(ready.at[p], ready_ref.at[p]) for p in parts]
    moves += [(scale, scale_ref), (router, router_ref)]
    copies = [pltpu.make_async_copy(*m, sem.at[i]) for i, m in enumerate(moves)]
    for c in copies:
        c.start()
    for c in copies:
        c.wait()


def solution(mesh):
    chips, banks = mesh.shape["zero"] // 2, mesh.shape["bank"]

    def per_device(train_down, router_weight, router_gain):
        experts, rows, lanes = train_down.shape
        per = rows // (2 * chips)
        columns = router_weight.shape[1]
        vmem = pl.BlockSpec(memory_space=pltpu.VMEM)
        hbm = pl.BlockSpec(memory_space=pltpu.HBM)
        n = len(PEERS)
        outs = (
            jax.ShapeDtypeStruct((experts, per, 2 * chips * lanes), jnp.bfloat16),
            jax.ShapeDtypeStruct((experts, per), jnp.float32),
            jax.ShapeDtypeStruct((columns * banks, 2 * chips * LANES), jnp.bfloat16),
        )
        held = [
            pltpu.with_memory_space_constraint(a, pltpu.HBM)
            for a in (train_down, router_weight.T, router_gain.reshape(1, -1))
        ]
        made = pl.pallas_call(
            functools.partial(exchange_kernel, (chips, banks)),
            out_shape=outs,
            in_specs=[hbm, hbm, hbm],
            out_specs=(vmem, vmem, vmem),
            scratch_shapes=[
                pltpu.VMEM((experts, rows, lanes), jnp.float32),
                pltpu.VMEM((columns, LANES), jnp.float32),
                pltpu.VMEM((1, LANES), jnp.float32),
                pltpu.VMEM((2 * chips, experts, per, lanes), jnp.bfloat16),
                pltpu.VMEM((EARLY, chips, LANES), jnp.float32),
                pltpu.VMEM((n, EARLY, chips, LANES), jnp.float32),
                pltpu.VMEM((EARLY, chips, LANES), jnp.float32),
                pltpu.VMEM((2, chips, HALF, LANES), jnp.float32),
                pltpu.VMEM((chips, HALF, LANES), jnp.float32),
                pltpu.VMEM((chips, HALF, LANES), jnp.float32),
                pltpu.VMEM((chips - 1, HALF, LANES), jnp.float32),
                pltpu.VMEM((2, chips, HALF, LANES), jnp.float32),
                pltpu.VMEM((2, columns * banks, chips * LANES), jnp.bfloat16),
                pltpu.SemaphoreType.DMA((experts + 2,)),
                pltpu.SemaphoreType.DMA((BLOCKS + 1,)),
                pltpu.SemaphoreType.DMA((BLOCKS + 1,)),
            ],
            compiler_params=pltpu.CompilerParams(
                collective_id=0, has_side_effects=True, vmem_limit_bytes=24 * 2**20
            ),
            name="exchange",
        )(*held)
        ready, scale, router = pl.pallas_call(
            store_kernel,
            out_shape=outs,
            in_specs=[vmem, vmem, vmem],
            out_specs=(hbm, hbm, hbm),
            scratch_shapes=[pltpu.SemaphoreType.DMA((STORES + 2,))],
            compiler_params=pltpu.CompilerParams(vmem_limit_bytes=4 * 2**20),
            name="store",
        )(*(pltpu.with_memory_space_constraint(a, pltpu.VMEM) for a in made))
        return ready, scale, router.T

    return jax.shard_map(
        per_device,
        mesh=mesh,
        in_specs=(P(("unit", "bank"), None, "zero"), P(("unit", "zero"), "bank"), P(("unit", "zero"))),
        out_specs=(P(("unit", "bank"), "zero", None), P(("unit", "bank"), "zero"), P("unit", None)),
        check_vma=False,
    )
```

```python
import functools

import jax
import jax.numpy as jnp
from jax import lax
from jax.experimental import pallas as pl
from jax.experimental.pallas import tpu as pltpu
from jax.sharding import PartitionSpec as P

MESH = pl.DeviceIdType.MESH
LANES = 128
HALF = 8
EARLY = 2
GROUP = 2
TAIL = 6
TIERS = (0, 2, 4)
STORES = 8

PEERS = [(d, c) for c in (1, 0) for d in (4, 3, 5, 2, 6, 1, 7)] + [(0, 1)]
ALIKE = [k for k, (d, c) in enumerate(PEERS) if c == 0]
PARTNER = len(PEERS) - 1
FIRST, PEAKS, SCALES, ROUTER, PAIR, PASS, SIDE, WHOLE, BLOCKS = range(9)


def exchange_kernel(
    units,
    x_ref, w_ref, g_ref,
    ready_ref, scale_ref, router_ref,
    xv, wv, gv, sent, early, early_in, early_scale,
    peaks, pair_in, merged, peaks_in, scales, tiles,
    x_sem, send_sem, recv_sem,
):
    chips, banks = units
    experts, rows, _ = x_ref.shape
    per = ready_ref.shape[1]
    me = lax.axis_index("zero")
    chip, core = me // 2, lax.rem(me, 2)
    bank = lax.axis_index("bank")
    mine = pl.ds(pl.multiple_of(me * LANES, LANES), LANES)
    every = range(len(PEERS))

    def peer(k):
        ahead, other = PEERS[k]
        chip_to = lax.rem(chip + ahead, chips)
        core_to = lax.rem(core + other, 2)
        return chip_to, {"zero": chip_to * 2 + core_to}

    def load(e):
        return pltpu.make_async_copy(x_ref.at[e], xv.at[e], x_sem.at[e])

    for e in range(experts):
        load(e).start()
    weight_in = pltpu.make_async_copy(w_ref, wv, x_sem.at[experts])
    gain_in = pltpu.make_async_copy(g_ref, gv, x_sem.at[experts + 1])
    weight_in.start()
    gain_in.start()

    barrier = pltpu.get_barrier_semaphore()
    for k in every:
        pl.semaphore_signal(barrier, inc=1, device_id=peer(k)[1], device_id_type=MESH)
    for b in range(1, banks):
        to = lax.rem(bank + b, banks)
        pl.semaphore_signal(barrier, inc=1, device_id={"bank": to}, device_id_type=MESH)

    def peak(e, block):
        tile = jnp.abs(xv[e, pl.ds(block * LANES, LANES), :])
        return jnp.max(tile.T, axis=0, keepdims=True)

    for e in range(EARLY):
        load(e).wait()
        early[e] = jnp.concatenate([peak(e, b) for b in range(chips)], axis=0)

    def copy(src, dst, kind, k, to=None):
        return pltpu.make_async_remote_copy(
            src_ref=src, dst_ref=dst,
            send_sem=send_sem.at[kind], recv_sem=recv_sem.at[kind],
            device_id=peer(k)[1] if to is None else to, device_id_type=MESH,
        )

    def await_all(ref, sem):
        pltpu.make_async_copy(ref, ref, sem).wait()

    def early_copy(k):
        return copy(early, early_in.at[k], FIRST, k)

    def peaks_copy(k):
        return copy(merged.at[peer(k)[0]], peaks_in.at[ALIKE.index(k)], PEAKS, k)

    pair_copy = copy(peaks.at[1 - core], pair_in, PAIR, PARTNER)

    def scales_copy(k):
        place = scales.at[core, chip]
        return copy(place, place, SCALES, k)

    scales_pass = copy(scales.at[core], scales.at[core], PASS, PARTNER)
    rank = pl.ds(pl.multiple_of(bank * 16, 16), 16)
    column = pl.ds(pl.multiple_of(chip * LANES, LANES), LANES)
    sevenths = tiles.at[0, pl.ds(0, 16), pl.ds(0, (chips - 1) * LANES)]

    def router_copy(k):
        place = tiles.at[core, rank, column]
        return copy(place, place, ROUTER, k)

    def cross_copy(b):
        place = tiles.at[core, rank]
        return copy(place, place, SIDE, None, {"bank": lax.rem(bank + b, banks)})

    router_pass = copy(tiles.at[core], tiles.at[core], WHOLE, PARTNER)

    def block_copy(e0, n, k):
        to = peer(k)[1]
        experts_of = pl.ds(e0, n)
        return copy(sent.at[to["zero"], experts_of], ready_ref.at[experts_of, :, mine], BLOCKS, k)

    pl.semaphore_wait(barrier, len(PEERS) + banks - 1)
    for k in every:
        early_copy(k).start()
    for e in range(EARLY, experts):
        load(e).wait()

    def half_peaks(half):
        @pl.loop(0, chips)
        def _(block):
            found = [peak(half * HALF + i, block) for i in range(HALF)]
            peaks[half, block] = jnp.concatenate(found, axis=0)

    half_peaks(1 - core)
    pair_copy.start()
    half_peaks(core)
    pair_copy.wait_recv()
    merged[...] = jnp.maximum(peaks[core], pair_in[...])
    for k in ALIKE:
        peaks_copy(k).start()
    weight_in.wait()
    gain_in.wait()
    tiles[core, rank, column] = (wv[...] * gv[...]).astype(jnp.bfloat16)
    for k in ALIKE:
        router_copy(k).start()

    def scaled(e, row_of):
        for b in range(chips):
            inverse = 1.0 / row_of(b)
            spread = jnp.broadcast_to(inverse, (LANES, LANES)).T
            y = (xv[e, pl.ds(b * LANES, LANES), :] * spread).astype(jnp.bfloat16)
            sent[2 * b, e] = y[:per]
            sent[2 * b + 1, e] = y[per:]
        ready_ref[e, :, mine] = sent[me, e]

    await_all(early_in, recv_sem.at[FIRST])
    top = early[...]
    for k in every:
        top = jnp.maximum(top, early_in[k])
    early_scale[...] = top
    for e in range(EARLY):
        scaled(e, lambda b: early_scale[e, b : b + 1, :])
        if e == 0:
            for k in every[:7]:
                block_copy(0, 1, k).start()
    await_all(peaks_in, recv_sem.at[PEAKS])
    top = merged[chip]
    for k in ALIKE:
        top = jnp.maximum(top, peaks_in[ALIKE.index(k)])
    scales[core, chip] = top
    for k in ALIKE:
        scales_copy(k).start()
    for k in every[7:]:
        block_copy(0, 1, k).start()
    for k in every:
        block_copy(1, EARLY - 1, k).start()
    await_all(sevenths, recv_sem.at[ROUTER])
    for b in range(1, banks):
        cross_copy(b).start()
    await_all(peaks_in, recv_sem.at[SCALES])
    scales_pass.start()
    scales_pass.wait_recv()
    def scale_group(e0):
        for j in range(GROUP):
            e = e0 + j
            scaled(e, lambda b: scales[e // HALF, b, pl.ds(lax.rem(e, HALF), 1), :])

    tail = experts - TAIL

    @pl.loop(0, (tail - EARLY) // GROUP)
    def _(i):
        scale_group(EARLY + i * GROUP)
        for k in every:
            block_copy(EARLY + i * GROUP, GROUP, k).start()

    pl.loop(0, TAIL // GROUP)(lambda i: scale_group(tail + i * GROUP))

    def tail_blocks(first, past):
        @pl.loop(0, TAIL // GROUP)
        def _(i):
            for k in every:
                to = peer(k)[0]

                @pl.when((to >= first) & (to < past))
                def _():
                    block_copy(tail + i * GROUP, GROUP, k).start()

    for first, past in zip(TIERS, TIERS[1:] + (chips,)):
        tail_blocks(first, past)

    whole = jnp.concatenate([scales[0, chip], scales[1, chip]], axis=0)
    scale_ref[...] = jnp.where(core == 0, whole[:, :per], whole[:, per:])
    await_all(tiles.at[core, pl.ds(0, 16 * (banks - 1))], recv_sem.at[SIDE])
    router_pass.start()
    router_pass.wait()
    for j in range(chips):
        for c in range(2):
            at = (2 * j + c) * LANES
            router_ref[:, at : at + LANES] = tiles[c, :, j * LANES : (j + 1) * LANES]
    await_all(early_in, send_sem.at[FIRST])
    await_all(peaks_in, send_sem.at[PEAKS])
    await_all(peaks_in, send_sem.at[SCALES])
    await_all(sevenths, send_sem.at[ROUTER])
    await_all(tiles.at[core, pl.ds(0, 16 * (banks - 1))], send_sem.at[SIDE])
    pair_copy.wait_send()
    scales_pass.wait_send()
    blocks = sent.at[pl.ds(0, len(PEERS))]
    await_all(blocks, send_sem.at[BLOCKS])
    await_all(blocks, recv_sem.at[BLOCKS])


def store_kernel(ready, scale, router, ready_ref, scale_ref, router_ref, sem):
    step = ready.shape[0] // STORES
    parts = [pl.ds(i * step, step) for i in range(STORES)]
    moves = [(ready.at[p], ready_ref.at[p]) for p in parts]
    moves += [(scale, scale_ref), (router, router_ref)]
    copies = [pltpu.make_async_copy(*m, sem.at[i]) for i, m in enumerate(moves)]
    for c in copies:
        c.start()
    for c in copies:
        c.wait()


def solution(mesh):
    chips, banks = mesh.shape["zero"] // 2, mesh.shape["bank"]

    def per_device(train_down, router_weight, router_gain):
        experts, rows, lanes = train_down.shape
        per = rows // (2 * chips)
        columns = router_weight.shape[1]
        vmem = pl.BlockSpec(memory_space=pltpu.VMEM)
        hbm = pl.BlockSpec(memory_space=pltpu.HBM)
        n = len(PEERS)
        outs = (
            jax.ShapeDtypeStruct((experts, per, 2 * chips * lanes), jnp.bfloat16),
            jax.ShapeDtypeStruct((experts, per), jnp.float32),
            jax.ShapeDtypeStruct((columns * banks, 2 * chips * LANES), jnp.bfloat16),
        )
        held = [
            pltpu.with_memory_space_constraint(a, pltpu.HBM)
            for a in (train_down, router_weight.T, router_gain.reshape(1, -1))
        ]
        made = pl.pallas_call(
            functools.partial(exchange_kernel, (chips, banks)),
            out_shape=outs,
            in_specs=[hbm, hbm, hbm],
            out_specs=(vmem, vmem, vmem),
            scratch_shapes=[
                pltpu.VMEM((experts, rows, lanes), jnp.float32),
                pltpu.VMEM((columns, LANES), jnp.float32),
                pltpu.VMEM((1, LANES), jnp.float32),
                pltpu.VMEM((2 * chips, experts, per, lanes), jnp.bfloat16),
                pltpu.VMEM((EARLY, chips, LANES), jnp.float32),
                pltpu.VMEM((n, EARLY, chips, LANES), jnp.float32),
                pltpu.VMEM((EARLY, chips, LANES), jnp.float32),
                pltpu.VMEM((2, chips, HALF, LANES), jnp.float32),
                pltpu.VMEM((chips, HALF, LANES), jnp.float32),
                pltpu.VMEM((chips, HALF, LANES), jnp.float32),
                pltpu.VMEM((chips - 1, HALF, LANES), jnp.float32),
                pltpu.VMEM((2, chips, HALF, LANES), jnp.float32),
                pltpu.VMEM((2, columns * banks, chips * LANES), jnp.bfloat16),
                pltpu.SemaphoreType.DMA((experts + 2,)),
                pltpu.SemaphoreType.DMA((BLOCKS + 1,)),
                pltpu.SemaphoreType.DMA((BLOCKS + 1,)),
            ],
            compiler_params=pltpu.CompilerParams(
                collective_id=0, has_side_effects=True, vmem_limit_bytes=24 * 2**20
            ),
            name="exchange",
        )(*held)
        ready, scale, router = pl.pallas_call(
            store_kernel,
            out_shape=outs,
            in_specs=[vmem, vmem, vmem],
            out_specs=(hbm, hbm, hbm),
            scratch_shapes=[pltpu.SemaphoreType.DMA((STORES + 2,))],
            compiler_params=pltpu.CompilerParams(vmem_limit_bytes=4 * 2**20),
            name="store",
        )(*(pltpu.with_memory_space_constraint(a, pltpu.VMEM) for a in made))
        return ready, scale, router.T

    return jax.shard_map(
        per_device,
        mesh=mesh,
        in_specs=(P(("unit", "bank"), None, "zero"), P(("unit", "zero"), "bank"), P(("unit", "zero"))),
        out_specs=(P(("unit", "bank"), "zero", None), P(("unit", "bank"), "zero"), P("unit", None)),
        check_vma=False,
    )
```

```python
import functools

import jax
import jax.numpy as jnp
from jax import lax
from jax.experimental import pallas as pl
from jax.experimental.pallas import tpu as pltpu
from jax.sharding import PartitionSpec as P

MESH = pl.DeviceIdType.MESH
LANES = 128
HALF = 8
EARLY = 2
GROUP = 2
TAIL = 6
TIERS = (0, 2, 4)
STORES = 8

PEERS = [(d, c) for c in (1, 0) for d in (4, 3, 5, 2, 6, 1, 7)] + [(0, 1)]
ALIKE = [k for k, (d, c) in enumerate(PEERS) if c == 0]
PARTNER = len(PEERS) - 1
FIRST, SECOND, PEAKS, SCALES, ROUTER, PAIR, PASS, SIDE, WHOLE, BLOCKS = range(10)


def exchange_kernel(
    units,
    x_ref, w_ref, g_ref,
    ready_ref, scale_ref, router_ref,
    xv, wv, gv, sent, early, early_in, early_scale,
    peaks, pair_in, merged, peaks_in, scales, tiles,
    x_sem, send_sem, recv_sem,
):
    chips, banks = units
    experts, rows, _ = x_ref.shape
    per = ready_ref.shape[1]
    me = lax.axis_index("zero")
    chip, core = me // 2, lax.rem(me, 2)
    bank = lax.axis_index("bank")
    mine = pl.ds(pl.multiple_of(me * LANES, LANES), LANES)
    every = range(len(PEERS))

    def peer(k):
        ahead, other = PEERS[k]
        chip_to = lax.rem(chip + ahead, chips)
        core_to = lax.rem(core + other, 2)
        return chip_to, {"zero": chip_to * 2 + core_to}

    def load(e):
        return pltpu.make_async_copy(x_ref.at[e], xv.at[e], x_sem.at[e])

    for e in range(experts):
        load(e).start()
    weight_in = pltpu.make_async_copy(w_ref, wv, x_sem.at[experts])
    gain_in = pltpu.make_async_copy(g_ref, gv, x_sem.at[experts + 1])
    weight_in.start()
    gain_in.start()

    barrier = pltpu.get_barrier_semaphore()
    for k in every:
        pl.semaphore_signal(barrier, inc=1, device_id=peer(k)[1], device_id_type=MESH)
    for b in range(1, banks):
        to = lax.rem(bank + b, banks)
        pl.semaphore_signal(barrier, inc=1, device_id={"bank": to}, device_id_type=MESH)

    def peak(e, block):
        tile = jnp.abs(xv[e, pl.ds(block * LANES, LANES), :])
        return jnp.max(tile.T, axis=0, keepdims=True)

    for e in range(EARLY):
        load(e).wait()
        early[e] = jnp.concatenate([peak(e, b) for b in range(chips)], axis=0)

    def copy(src, dst, kind, k, to=None):
        return pltpu.make_async_remote_copy(
            src_ref=src, dst_ref=dst,
            send_sem=send_sem.at[kind], recv_sem=recv_sem.at[kind],
            device_id=peer(k)[1] if to is None else to, device_id_type=MESH,
        )

    def await_all(ref, sem):
        pltpu.make_async_copy(ref, ref, sem).wait()

    def early_copy(i, k):
        return copy(early.at[i], early_in.at[i, k], FIRST + i, k)

    def peaks_copy(k):
        return copy(merged.at[peer(k)[0]], peaks_in.at[ALIKE.index(k)], PEAKS, k)

    pair_copy = copy(peaks.at[1 - core], pair_in, PAIR, PARTNER)

    def scales_copy(k):
        place = scales.at[core, chip]
        return copy(place, place, SCALES, k)

    scales_pass = copy(scales.at[core], scales.at[core], PASS, PARTNER)
    rank = pl.ds(pl.multiple_of(bank * 16, 16), 16)
    column = pl.ds(pl.multiple_of(chip * LANES, LANES), LANES)
    sevenths = tiles.at[0, pl.ds(0, 16), pl.ds(0, (chips - 1) * LANES)]

    def router_copy(k):
        place = tiles.at[core, rank, column]
        return copy(place, place, ROUTER, k)

    def cross_copy(b):
        place = tiles.at[core, rank]
        return copy(place, place, SIDE, None, {"bank": lax.rem(bank + b, banks)})

    router_pass = copy(tiles.at[core], tiles.at[core], WHOLE, PARTNER)

    def block_copy(e0, n, k):
        to = peer(k)[1]
        experts_of = pl.ds(e0, n)
        return copy(sent.at[to["zero"], experts_of], ready_ref.at[experts_of, :, mine], BLOCKS, k)

    pl.semaphore_wait(barrier, len(PEERS) + banks - 1)
    for i in range(EARLY):
        for k in every:
            early_copy(i, k).start()
    for e in range(EARLY, experts):
        load(e).wait()

    def half_peaks(half):
        @pl.loop(0, chips)
        def _(block):
            found = [peak(half * HALF + i, block) for i in range(HALF)]
            peaks[half, block] = jnp.concatenate(found, axis=0)

    half_peaks(1 - core)
    pair_copy.start()
    half_peaks(core)
    pair_copy.wait_recv()
    merged[...] = jnp.maximum(peaks[core], pair_in[...])
    for k in ALIKE:
        peaks_copy(k).start()
    weight_in.wait()
    gain_in.wait()
    tiles[core, rank, column] = (wv[...] * gv[...]).astype(jnp.bfloat16)
    for k in ALIKE:
        router_copy(k).start()

    def scaled(e, row_of):
        for b in range(chips):
            inverse = 1.0 / row_of(b)
            spread = jnp.broadcast_to(inverse, (LANES, LANES)).T
            y = (xv[e, pl.ds(b * LANES, LANES), :] * spread).astype(jnp.bfloat16)
            sent[2 * b, e] = y[:per]
            sent[2 * b + 1, e] = y[per:]
        ready_ref[e, :, mine] = sent[me, e]

    for e in range(EARLY):
        await_all(early_in.at[e], recv_sem.at[FIRST + e])
        early_scale[e] = functools.reduce(jnp.maximum, [early_in[e, k] for k in every], early[e])
        scaled(e, lambda b: early_scale[e, b : b + 1, :])
        if e == 0:
            for k in every[:7]:
                block_copy(0, 1, k).start()
    await_all(peaks_in, recv_sem.at[PEAKS])
    top = merged[chip]
    for k in ALIKE:
        top = jnp.maximum(top, peaks_in[ALIKE.index(k)])
    scales[core, chip] = top
    for k in ALIKE:
        scales_copy(k).start()
    for k in every[7:]:
        block_copy(0, 1, k).start()
    for k in every:
        block_copy(1, EARLY - 1, k).start()
    await_all(sevenths, recv_sem.at[ROUTER])
    for b in range(1, banks):
        cross_copy(b).start()
    await_all(peaks_in, recv_sem.at[SCALES])
    scales_pass.start()
    scales_pass.wait_recv()
    def scale_group(e0):
        for j in range(GROUP):
            e = e0 + j
            scaled(e, lambda b: scales[e // HALF, b, pl.ds(lax.rem(e, HALF), 1), :])

    tail = experts - TAIL

    @pl.loop(0, (tail - EARLY) // GROUP)
    def _(i):
        scale_group(EARLY + i * GROUP)
        for k in every:
            block_copy(EARLY + i * GROUP, GROUP, k).start()

    pl.loop(0, TAIL // GROUP)(lambda i: scale_group(tail + i * GROUP))

    def tail_blocks(first, past):
        @pl.loop(0, TAIL // GROUP)
        def _(i):
            for k in every:
                to = peer(k)[0]

                @pl.when((to >= first) & (to < past))
                def _():
                    block_copy(tail + i * GROUP, GROUP, k).start()

    for first, past in zip(TIERS, TIERS[1:] + (chips,)):
        tail_blocks(first, past)

    whole = jnp.concatenate([scales[0, chip], scales[1, chip]], axis=0)
    scale_ref[...] = jnp.where(core == 0, whole[:, :per], whole[:, per:])
    await_all(tiles.at[core, pl.ds(0, 16 * (banks - 1))], recv_sem.at[SIDE])
    router_pass.start()
    router_pass.wait()
    for j in range(chips):
        for c in range(2):
            at = (2 * j + c) * LANES
            router_ref[:, at : at + LANES] = tiles[c, :, j * LANES : (j + 1) * LANES]
    for e in range(EARLY):
        await_all(early_in.at[e], send_sem.at[FIRST + e])
    await_all(peaks_in, send_sem.at[PEAKS])
    await_all(peaks_in, send_sem.at[SCALES])
    await_all(sevenths, send_sem.at[ROUTER])
    await_all(tiles.at[core, pl.ds(0, 16 * (banks - 1))], send_sem.at[SIDE])
    pair_copy.wait_send()
    scales_pass.wait_send()
    blocks = sent.at[pl.ds(0, len(PEERS))]
    await_all(blocks, send_sem.at[BLOCKS])
    await_all(blocks, recv_sem.at[BLOCKS])


def store_kernel(ready, scale, router, ready_ref, scale_ref, router_ref, sem):
    step = ready.shape[0] // STORES
    parts = [pl.ds(i * step, step) for i in range(STORES)]
    moves = [(ready.at[p], ready_ref.at[p]) for p in parts]
    moves += [(scale, scale_ref), (router, router_ref)]
    copies = [pltpu.make_async_copy(*m, sem.at[i]) for i, m in enumerate(moves)]
    for c in copies:
        c.start()
    for c in copies:
        c.wait()


def solution(mesh):
    chips, banks = mesh.shape["zero"] // 2, mesh.shape["bank"]

    def per_device(train_down, router_weight, router_gain):
        experts, rows, lanes = train_down.shape
        per = rows // (2 * chips)
        columns = router_weight.shape[1]
        vmem = pl.BlockSpec(memory_space=pltpu.VMEM)
        hbm = pl.BlockSpec(memory_space=pltpu.HBM)
        n = len(PEERS)
        outs = (
            jax.ShapeDtypeStruct((experts, per, 2 * chips * lanes), jnp.bfloat16),
            jax.ShapeDtypeStruct((experts, per), jnp.float32),
            jax.ShapeDtypeStruct((columns * banks, 2 * chips * LANES), jnp.bfloat16),
        )
        held = [
            pltpu.with_memory_space_constraint(a, pltpu.HBM)
            for a in (train_down, router_weight.T, router_gain.reshape(1, -1))
        ]
        made = pl.pallas_call(
            functools.partial(exchange_kernel, (chips, banks)),
            out_shape=outs,
            in_specs=[hbm, hbm, hbm],
            out_specs=(vmem, vmem, vmem),
            scratch_shapes=[
                pltpu.VMEM((experts, rows, lanes), jnp.float32),
                pltpu.VMEM((columns, LANES), jnp.float32),
                pltpu.VMEM((1, LANES), jnp.float32),
                pltpu.VMEM((2 * chips, experts, per, lanes), jnp.bfloat16),
                pltpu.VMEM((EARLY, chips, LANES), jnp.float32),
                pltpu.VMEM((EARLY, n, chips, LANES), jnp.float32),
                pltpu.VMEM((EARLY, chips, LANES), jnp.float32),
                pltpu.VMEM((2, chips, HALF, LANES), jnp.float32),
                pltpu.VMEM((chips, HALF, LANES), jnp.float32),
                pltpu.VMEM((chips, HALF, LANES), jnp.float32),
                pltpu.VMEM((chips - 1, HALF, LANES), jnp.float32),
                pltpu.VMEM((2, chips, HALF, LANES), jnp.float32),
                pltpu.VMEM((2, columns * banks, chips * LANES), jnp.bfloat16),
                pltpu.SemaphoreType.DMA((experts + 2,)),
                pltpu.SemaphoreType.DMA((BLOCKS + 1,)),
                pltpu.SemaphoreType.DMA((BLOCKS + 1,)),
            ],
            compiler_params=pltpu.CompilerParams(
                collective_id=0, has_side_effects=True, vmem_limit_bytes=24 * 2**20
            ),
            name="exchange",
        )(*held)
        ready, scale, router = pl.pallas_call(
            store_kernel,
            out_shape=outs,
            in_specs=[vmem, vmem, vmem],
            out_specs=(hbm, hbm, hbm),
            scratch_shapes=[pltpu.SemaphoreType.DMA((STORES + 2,))],
            compiler_params=pltpu.CompilerParams(vmem_limit_bytes=4 * 2**20),
            name="store",
        )(*(pltpu.with_memory_space_constraint(a, pltpu.VMEM) for a in made))
        return ready, scale, router.T

    return jax.shard_map(
        per_device,
        mesh=mesh,
        in_specs=(P(("unit", "bank"), None, "zero"), P(("unit", "zero"), "bank"), P(("unit", "zero"))),
        out_specs=(P(("unit", "bank"), "zero", None), P(("unit", "bank"), "zero"), P("unit", None)),
        check_vma=False,
    )
```

```python
import functools

import jax
import jax.numpy as jnp
from jax import lax
from jax.experimental import pallas as pl
from jax.experimental.pallas import tpu as pltpu
from jax.sharding import PartitionSpec as P

MESH = pl.DeviceIdType.MESH
LANES = 128
HALF = 8
EARLY = 2
GROUP = 2
TAIL = 6
TIERS = (0, 2, 4)
STORES = 8

PEERS = [(d, c) for c in (1, 0) for d in (4, 3, 5, 2, 6, 1, 7)] + [(0, 1)]
ALIKE = [k for k, (d, c) in enumerate(PEERS) if c == 0]
PARTNER = len(PEERS) - 1
FIRST, SECOND, PEAKS, SCALES, ROUTER, PAIR, PASS, SIDE, WHOLE, BLOCKS = range(10)


def exchange_kernel(
    units,
    x_ref, w_ref, g_ref,
    ready_ref, scale_ref, router_ref,
    xv, wv, gv, sent, early, early_in, early_scale,
    peaks, pair_in, merged, peaks_in, scales, tiles,
    x_sem, send_sem, recv_sem,
):
    chips, banks = units
    experts, rows, _ = x_ref.shape
    per = ready_ref.shape[1]
    me = lax.axis_index("zero")
    chip, core = me // 2, lax.rem(me, 2)
    bank = lax.axis_index("bank")
    mine = pl.ds(pl.multiple_of(me * LANES, LANES), LANES)
    every = range(len(PEERS))

    def peer(k):
        ahead, other = PEERS[k]
        chip_to = lax.rem(chip + ahead, chips)
        core_to = lax.rem(core + other, 2)
        return chip_to, {"zero": chip_to * 2 + core_to}

    def load(e):
        return pltpu.make_async_copy(x_ref.at[e], xv.at[e], x_sem.at[e])

    for e in range(experts):
        load(e).start()
    weight_in = pltpu.make_async_copy(w_ref, wv, x_sem.at[experts])
    gain_in = pltpu.make_async_copy(g_ref, gv, x_sem.at[experts + 1])
    weight_in.start()
    gain_in.start()

    barrier = pltpu.get_barrier_semaphore()
    for k in every:
        pl.semaphore_signal(barrier, inc=1, device_id=peer(k)[1], device_id_type=MESH)
    for b in range(1, banks):
        to = lax.rem(bank + b, banks)
        pl.semaphore_signal(barrier, inc=1, device_id={"bank": to}, device_id_type=MESH)

    def peak(e, block):
        tile = jnp.abs(xv[e, pl.ds(block * LANES, LANES), :])
        return jnp.max(tile.T, axis=0, keepdims=True)

    for e in range(EARLY):
        load(e).wait()
        early[e] = jnp.concatenate([peak(e, b) for b in range(chips)], axis=0)

    def copy(src, dst, kind, k, to=None):
        return pltpu.make_async_remote_copy(
            src_ref=src, dst_ref=dst,
            send_sem=send_sem.at[kind], recv_sem=recv_sem.at[kind],
            device_id=peer(k)[1] if to is None else to, device_id_type=MESH,
        )

    def await_all(ref, sem):
        pltpu.make_async_copy(ref, ref, sem).wait()

    def early_copy(i, k):
        return copy(early.at[i], early_in.at[i, k], FIRST + i, k)

    def peaks_copy(k):
        return copy(merged.at[peer(k)[0]], peaks_in.at[ALIKE.index(k)], PEAKS, k)

    pair_copy = copy(peaks.at[1 - core], pair_in, PAIR, PARTNER)

    def scales_copy(k):
        place = scales.at[core, chip]
        return copy(place, place, SCALES, k)

    scales_pass = copy(scales.at[core], scales.at[core], PASS, PARTNER)
    rank = pl.ds(pl.multiple_of(bank * 16, 16), 16)
    column = pl.ds(pl.multiple_of(chip * LANES, LANES), LANES)
    sevenths = tiles.at[0, pl.ds(0, 16), pl.ds(0, (chips - 1) * LANES)]

    def router_copy(k):
        place = tiles.at[core, rank, column]
        return copy(place, place, ROUTER, k)

    def cross_copy(b):
        place = tiles.at[core, rank]
        return copy(place, place, SIDE, None, {"bank": lax.rem(bank + b, banks)})

    router_pass = copy(tiles.at[core], tiles.at[core], WHOLE, PARTNER)

    def block_copy(e0, n, k):
        to = peer(k)[1]
        experts_of = pl.ds(e0, n)
        return copy(sent.at[to["zero"], experts_of], ready_ref.at[experts_of, :, mine], BLOCKS, k)

    pl.semaphore_wait(barrier, len(PEERS) + banks - 1)
    for i in range(EARLY):
        for k in every:
            early_copy(i, k).start()
    for e in range(EARLY, experts):
        load(e).wait()

    def half_peaks(half):
        @pl.loop(0, chips // 2)
        def _(pair):
            for block in (2 * pair, 2 * pair + 1):
                found = [peak(half * HALF + i, block) for i in range(HALF)]
                peaks[half, block] = jnp.concatenate(found, axis=0)

    half_peaks(1 - core)
    pair_copy.start()
    half_peaks(core)
    pair_copy.wait_recv()
    merged[...] = jnp.maximum(peaks[core], pair_in[...])
    for k in ALIKE:
        peaks_copy(k).start()
    weight_in.wait()
    gain_in.wait()
    tiles[core, rank, column] = (wv[...] * gv[...]).astype(jnp.bfloat16)
    for k in ALIKE:
        router_copy(k).start()

    def scaled(e, row_of):
        for b in range(chips):
            inverse = 1.0 / row_of(b)
            spread = jnp.broadcast_to(inverse, (LANES, LANES)).T
            y = (xv[e, pl.ds(b * LANES, LANES), :] * spread).astype(jnp.bfloat16)
            sent[2 * b, e] = y[:per]
            sent[2 * b + 1, e] = y[per:]
        ready_ref[e, :, mine] = sent[me, e]

    def early_scaled(e):
        await_all(early_in.at[e], recv_sem.at[FIRST + e])
        early_scale[e] = functools.reduce(jnp.maximum, [early_in[e, k] for k in every], early[e])
        scaled(e, lambda b: early_scale[e, b : b + 1, :])

    early_scaled(0)
    for k in every[:7]:
        block_copy(0, 1, k).start()
    await_all(peaks_in, recv_sem.at[PEAKS])
    top = merged[chip]
    for k in ALIKE:
        top = jnp.maximum(top, peaks_in[ALIKE.index(k)])
    scales[core, chip] = top
    for k in ALIKE:
        scales_copy(k).start()
    for k in every[7:]:
        block_copy(0, 1, k).start()
    early_scaled(1)
    for k in every:
        block_copy(1, EARLY - 1, k).start()
    await_all(sevenths, recv_sem.at[ROUTER])
    for b in range(1, banks):
        cross_copy(b).start()
    await_all(peaks_in, recv_sem.at[SCALES])
    scales_pass.start()
    scales_pass.wait_recv()
    def scale_group(e0):
        for j in range(GROUP):
            e = e0 + j
            scaled(e, lambda b: scales[e // HALF, b, pl.ds(lax.rem(e, HALF), 1), :])

    tail = experts - TAIL

    @pl.loop(0, (tail - EARLY) // GROUP)
    def _(i):
        scale_group(EARLY + i * GROUP)
        for k in every:
            block_copy(EARLY + i * GROUP, GROUP, k).start()

    pl.loop(0, TAIL // GROUP)(lambda i: scale_group(tail + i * GROUP))

    def tail_blocks(first, past):
        @pl.loop(0, TAIL // GROUP)
        def _(i):
            for k in every:
                to = peer(k)[0]

                @pl.when((to >= first) & (to < past))
                def _():
                    block_copy(tail + i * GROUP, GROUP, k).start()

    for first, past in zip(TIERS, TIERS[1:] + (chips,)):
        tail_blocks(first, past)

    whole = jnp.concatenate([scales[0, chip], scales[1, chip]], axis=0)
    scale_ref[...] = jnp.where(core == 0, whole[:, :per], whole[:, per:])
    await_all(tiles.at[core, pl.ds(0, 16 * (banks - 1))], recv_sem.at[SIDE])
    router_pass.start()
    router_pass.wait()
    for j in range(chips):
        for c in range(2):
            at = (2 * j + c) * LANES
            router_ref[:, at : at + LANES] = tiles[c, :, j * LANES : (j + 1) * LANES]
    for e in range(EARLY):
        await_all(early_in.at[e], send_sem.at[FIRST + e])
    await_all(peaks_in, send_sem.at[PEAKS])
    await_all(peaks_in, send_sem.at[SCALES])
    await_all(sevenths, send_sem.at[ROUTER])
    await_all(tiles.at[core, pl.ds(0, 16 * (banks - 1))], send_sem.at[SIDE])
    pair_copy.wait_send()
    scales_pass.wait_send()
    blocks = sent.at[pl.ds(0, len(PEERS))]
    await_all(blocks, send_sem.at[BLOCKS])
    await_all(blocks, recv_sem.at[BLOCKS])


def store_kernel(ready, scale, router, ready_ref, scale_ref, router_ref, sem):
    step = ready.shape[0] // STORES
    parts = [pl.ds(i * step, step) for i in range(STORES)]
    moves = [(ready.at[p], ready_ref.at[p]) for p in parts]
    moves += [(scale, scale_ref), (router, router_ref)]
    copies = [pltpu.make_async_copy(*m, sem.at[i]) for i, m in enumerate(moves)]
    for c in copies:
        c.start()
    for c in copies:
        c.wait()


def solution(mesh):
    chips, banks = mesh.shape["zero"] // 2, mesh.shape["bank"]

    def per_device(train_down, router_weight, router_gain):
        experts, rows, lanes = train_down.shape
        per = rows // (2 * chips)
        columns = router_weight.shape[1]
        vmem = pl.BlockSpec(memory_space=pltpu.VMEM)
        hbm = pl.BlockSpec(memory_space=pltpu.HBM)
        n = len(PEERS)
        outs = (
            jax.ShapeDtypeStruct((experts, per, 2 * chips * lanes), jnp.bfloat16),
            jax.ShapeDtypeStruct((experts, per), jnp.float32),
            jax.ShapeDtypeStruct((columns * banks, 2 * chips * LANES), jnp.bfloat16),
        )
        held = [
            pltpu.with_memory_space_constraint(a, pltpu.HBM)
            for a in (train_down, router_weight.T, router_gain.reshape(1, -1))
        ]
        made = pl.pallas_call(
            functools.partial(exchange_kernel, (chips, banks)),
            out_shape=outs,
            in_specs=[hbm, hbm, hbm],
            out_specs=(vmem, vmem, vmem),
            scratch_shapes=[
                pltpu.VMEM((experts, rows, lanes), jnp.float32),
                pltpu.VMEM((columns, LANES), jnp.float32),
                pltpu.VMEM((1, LANES), jnp.float32),
                pltpu.VMEM((2 * chips, experts, per, lanes), jnp.bfloat16),
                pltpu.VMEM((EARLY, chips, LANES), jnp.float32),
                pltpu.VMEM((EARLY, n, chips, LANES), jnp.float32),
                pltpu.VMEM((EARLY, chips, LANES), jnp.float32),
                pltpu.VMEM((2, chips, HALF, LANES), jnp.float32),
                pltpu.VMEM((chips, HALF, LANES), jnp.float32),
                pltpu.VMEM((chips, HALF, LANES), jnp.float32),
                pltpu.VMEM((chips - 1, HALF, LANES), jnp.float32),
                pltpu.VMEM((2, chips, HALF, LANES), jnp.float32),
                pltpu.VMEM((2, columns * banks, chips * LANES), jnp.bfloat16),
                pltpu.SemaphoreType.DMA((experts + 2,)),
                pltpu.SemaphoreType.DMA((BLOCKS + 1,)),
                pltpu.SemaphoreType.DMA((BLOCKS + 1,)),
            ],
            compiler_params=pltpu.CompilerParams(
                collective_id=0, has_side_effects=True, vmem_limit_bytes=24 * 2**20
            ),
            name="exchange",
        )(*held)
        ready, scale, router = pl.pallas_call(
            store_kernel,
            out_shape=outs,
            in_specs=[vmem, vmem, vmem],
            out_specs=(hbm, hbm, hbm),
            scratch_shapes=[pltpu.SemaphoreType.DMA((STORES + 2,))],
            compiler_params=pltpu.CompilerParams(vmem_limit_bytes=4 * 2**20),
            name="store",
        )(*(pltpu.with_memory_space_constraint(a, pltpu.VMEM) for a in made))
        return ready, scale, router.T

    return jax.shard_map(
        per_device,
        mesh=mesh,
        in_specs=(P(("unit", "bank"), None, "zero"), P(("unit", "zero"), "bank"), P(("unit", "zero"))),
        out_specs=(P(("unit", "bank"), "zero", None), P(("unit", "bank"), "zero"), P("unit", None)),
        check_vma=False,
    )
```

```python
import functools

import jax
import jax.numpy as jnp
from jax import lax
from jax.experimental import pallas as pl
from jax.experimental.pallas import tpu as pltpu
from jax.sharding import PartitionSpec as P

MESH = pl.DeviceIdType.MESH
LANES = 128
HALF = 8
EARLY = 2
GROUP = 2
TAIL = 4
TIERS = (0, 2, 4)
STORES = 8

PEERS = [(d, c) for c in (1, 0) for d in (4, 3, 5, 2, 6, 1, 7)] + [(0, 1)]
ALIKE = [k for k, (d, c) in enumerate(PEERS) if c == 0]
PARTNER = len(PEERS) - 1
FIRST, SECOND, PEAKS, SCALES, ROUTER, PAIR, PASS, SIDE, WHOLE, BLOCKS = range(10)


def exchange_kernel(
    units,
    x_ref, w_ref, g_ref,
    ready_ref, scale_ref, router_ref,
    xv, wv, gv, sent, early, early_in, early_scale,
    peaks, pair_in, merged, peaks_in, scales, tiles,
    x_sem, send_sem, recv_sem,
):
    chips, banks = units
    experts, rows, _ = x_ref.shape
    per = ready_ref.shape[1]
    me = lax.axis_index("zero")
    chip, core = me // 2, lax.rem(me, 2)
    bank = lax.axis_index("bank")
    mine = pl.ds(pl.multiple_of(me * LANES, LANES), LANES)
    every = range(len(PEERS))

    def peer(k):
        ahead, other = PEERS[k]
        chip_to = lax.rem(chip + ahead, chips)
        core_to = lax.rem(core + other, 2)
        return chip_to, {"zero": chip_to * 2 + core_to}

    def load(e):
        return pltpu.make_async_copy(x_ref.at[e], xv.at[e], x_sem.at[e])

    for e in range(experts):
        load(e).start()
    weight_in = pltpu.make_async_copy(w_ref, wv, x_sem.at[experts])
    gain_in = pltpu.make_async_copy(g_ref, gv, x_sem.at[experts + 1])
    weight_in.start()
    gain_in.start()

    barrier = pltpu.get_barrier_semaphore()
    for k in every:
        pl.semaphore_signal(barrier, inc=1, device_id=peer(k)[1], device_id_type=MESH)
    for b in range(1, banks):
        to = lax.rem(bank + b, banks)
        pl.semaphore_signal(barrier, inc=1, device_id={"bank": to}, device_id_type=MESH)

    def peak(e, block):
        tile = jnp.abs(xv[e, pl.ds(block * LANES, LANES), :])
        return jnp.max(tile.T, axis=0, keepdims=True)

    for e in range(EARLY):
        load(e).wait()
        early[e] = jnp.concatenate([peak(e, b) for b in range(chips)], axis=0)

    def copy(src, dst, kind, k, to=None):
        return pltpu.make_async_remote_copy(
            src_ref=src, dst_ref=dst,
            send_sem=send_sem.at[kind], recv_sem=recv_sem.at[kind],
            device_id=peer(k)[1] if to is None else to, device_id_type=MESH,
        )

    def await_all(ref, sem):
        pltpu.make_async_copy(ref, ref, sem).wait()

    def early_copy(i, k):
        return copy(early.at[i], early_in.at[i, k], FIRST + i, k)

    def peaks_copy(k):
        return copy(merged.at[peer(k)[0]], peaks_in.at[ALIKE.index(k)], PEAKS, k)

    pair_copy = copy(peaks.at[1 - core], pair_in, PAIR, PARTNER)

    def scales_copy(k):
        place = scales.at[core, chip]
        return copy(place, place, SCALES, k)

    scales_pass = copy(scales.at[core], scales.at[core], PASS, PARTNER)
    rank = pl.ds(pl.multiple_of(bank * 16, 16), 16)
    column = pl.ds(pl.multiple_of(chip * LANES, LANES), LANES)
    sevenths = tiles.at[0, pl.ds(0, 16), pl.ds(0, (chips - 1) * LANES)]

    def router_copy(k):
        place = tiles.at[core, rank, column]
        return copy(place, place, ROUTER, k)

    def cross_copy(b):
        place = tiles.at[core, rank]
        return copy(place, place, SIDE, None, {"bank": lax.rem(bank + b, banks)})

    router_pass = copy(tiles.at[core], tiles.at[core], WHOLE, PARTNER)

    def block_copy(e0, n, k):
        to = peer(k)[1]
        experts_of = pl.ds(e0, n)
        return copy(sent.at[to["zero"], experts_of], ready_ref.at[experts_of, :, mine], BLOCKS, k)

    pl.semaphore_wait(barrier, len(PEERS) + banks - 1)
    for i in range(EARLY):
        for k in every:
            early_copy(i, k).start()
    for e in range(EARLY, experts):
        load(e).wait()

    def half_peaks(half):
        @pl.loop(0, chips // 2)
        def _(pair):
            for block in (2 * pair, 2 * pair + 1):
                found = [peak(half * HALF + i, block) for i in range(HALF)]
                peaks[half, block] = jnp.concatenate(found, axis=0)

    half_peaks(1 - core)
    pair_copy.start()
    half_peaks(core)
    pair_copy.wait_recv()
    merged[...] = jnp.maximum(peaks[core], pair_in[...])
    for k in ALIKE:
        peaks_copy(k).start()
    weight_in.wait()
    gain_in.wait()
    tiles[core, rank, column] = (wv[...] * gv[...]).astype(jnp.bfloat16)
    for k in ALIKE:
        router_copy(k).start()

    def scaled(e, row_of):
        for b in range(chips):
            inverse = 1.0 / row_of(b)
            spread = jnp.broadcast_to(inverse, (LANES, LANES)).T
            y = (xv[e, pl.ds(b * LANES, LANES), :] * spread).astype(jnp.bfloat16)
            sent[2 * b, e] = y[:per]
            sent[2 * b + 1, e] = y[per:]
        ready_ref[e, :, mine] = sent[me, e]

    def early_scaled(e):
        await_all(early_in.at[e], recv_sem.at[FIRST + e])
        early_scale[e] = functools.reduce(jnp.maximum, [early_in[e, k] for k in every], early[e])
        scaled(e, lambda b: early_scale[e, b : b + 1, :])

    early_scaled(0)
    for k in every[:7]:
        block_copy(0, 1, k).start()
    await_all(peaks_in, recv_sem.at[PEAKS])
    top = merged[chip]
    for k in ALIKE:
        top = jnp.maximum(top, peaks_in[ALIKE.index(k)])
    scales[core, chip] = top
    for k in ALIKE:
        scales_copy(k).start()
    for k in every[7:]:
        block_copy(0, 1, k).start()
    early_scaled(1)
    for k in every:
        block_copy(1, EARLY - 1, k).start()
    await_all(sevenths, recv_sem.at[ROUTER])
    for b in range(1, banks):
        cross_copy(b).start()
    await_all(peaks_in, recv_sem.at[SCALES])
    scales_pass.start()
    scales_pass.wait_recv()
    def scale_group(e0):
        for j in range(GROUP):
            e = e0 + j
            scaled(e, lambda b: scales[e // HALF, b, pl.ds(lax.rem(e, HALF), 1), :])

    tail = experts - TAIL

    @pl.loop(0, (tail - EARLY) // GROUP)
    def _(i):
        scale_group(EARLY + i * GROUP)
        for k in [PARTNER, *every[:PARTNER]]:
            block_copy(EARLY + i * GROUP, GROUP, k).start()

    pl.loop(0, TAIL // GROUP)(lambda i: scale_group(tail + i * GROUP))

    def tail_blocks(first, past):
        @pl.loop(0, TAIL // GROUP)
        def _(i):
            for k in every:
                to = peer(k)[0]

                @pl.when((to >= first) & (to < past))
                def _():
                    block_copy(tail + i * GROUP, GROUP, k).start()

    for first, past in zip(TIERS, TIERS[1:] + (chips,)):
        tail_blocks(first, past)

    whole = jnp.concatenate([scales[0, chip], scales[1, chip]], axis=0)
    scale_ref[...] = jnp.where(core == 0, whole[:, :per], whole[:, per:])
    await_all(tiles.at[core, pl.ds(0, 16 * (banks - 1))], recv_sem.at[SIDE])
    router_pass.start()
    router_pass.wait()
    for j in range(chips):
        for c in range(2):
            at = (2 * j + c) * LANES
            router_ref[:, at : at + LANES] = tiles[c, :, j * LANES : (j + 1) * LANES]
    for e in range(EARLY):
        await_all(early_in.at[e], send_sem.at[FIRST + e])
    await_all(peaks_in, send_sem.at[PEAKS])
    await_all(peaks_in, send_sem.at[SCALES])
    await_all(sevenths, send_sem.at[ROUTER])
    await_all(tiles.at[core, pl.ds(0, 16 * (banks - 1))], send_sem.at[SIDE])
    pair_copy.wait_send()
    scales_pass.wait_send()
    blocks = sent.at[pl.ds(0, len(PEERS))]
    await_all(blocks, send_sem.at[BLOCKS])
    await_all(blocks, recv_sem.at[BLOCKS])


def store_kernel(ready, scale, router, ready_ref, scale_ref, router_ref, sem):
    step = ready.shape[0] // STORES
    parts = [pl.ds(i * step, step) for i in range(STORES)]
    moves = [(ready.at[p], ready_ref.at[p]) for p in parts]
    moves += [(scale, scale_ref), (router, router_ref)]
    copies = [pltpu.make_async_copy(*m, sem.at[i]) for i, m in enumerate(moves)]
    for c in copies:
        c.start()
    for c in copies:
        c.wait()


def solution(mesh):
    chips, banks = mesh.shape["zero"] // 2, mesh.shape["bank"]

    def per_device(train_down, router_weight, router_gain):
        experts, rows, lanes = train_down.shape
        per = rows // (2 * chips)
        columns = router_weight.shape[1]
        vmem = pl.BlockSpec(memory_space=pltpu.VMEM)
        hbm = pl.BlockSpec(memory_space=pltpu.HBM)
        n = len(PEERS)
        outs = (
            jax.ShapeDtypeStruct((experts, per, 2 * chips * lanes), jnp.bfloat16),
            jax.ShapeDtypeStruct((experts, per), jnp.float32),
            jax.ShapeDtypeStruct((columns * banks, 2 * chips * LANES), jnp.bfloat16),
        )
        held = [
            pltpu.with_memory_space_constraint(a, pltpu.HBM)
            for a in (train_down, router_weight.T, router_gain.reshape(1, -1))
        ]
        made = pl.pallas_call(
            functools.partial(exchange_kernel, (chips, banks)),
            out_shape=outs,
            in_specs=[hbm, hbm, hbm],
            out_specs=(vmem, vmem, vmem),
            scratch_shapes=[
                pltpu.VMEM((experts, rows, lanes), jnp.float32),
                pltpu.VMEM((columns, LANES), jnp.float32),
                pltpu.VMEM((1, LANES), jnp.float32),
                pltpu.VMEM((2 * chips, experts, per, lanes), jnp.bfloat16),
                pltpu.VMEM((EARLY, chips, LANES), jnp.float32),
                pltpu.VMEM((EARLY, n, chips, LANES), jnp.float32),
                pltpu.VMEM((EARLY, chips, LANES), jnp.float32),
                pltpu.VMEM((2, chips, HALF, LANES), jnp.float32),
                pltpu.VMEM((chips, HALF, LANES), jnp.float32),
                pltpu.VMEM((chips, HALF, LANES), jnp.float32),
                pltpu.VMEM((chips - 1, HALF, LANES), jnp.float32),
                pltpu.VMEM((2, chips, HALF, LANES), jnp.float32),
                pltpu.VMEM((2, columns * banks, chips * LANES), jnp.bfloat16),
                pltpu.SemaphoreType.DMA((experts + 2,)),
                pltpu.SemaphoreType.DMA((BLOCKS + 1,)),
                pltpu.SemaphoreType.DMA((BLOCKS + 1,)),
            ],
            compiler_params=pltpu.CompilerParams(
                collective_id=0, has_side_effects=True, vmem_limit_bytes=24 * 2**20
            ),
            name="exchange",
        )(*held)
        ready, scale, router = pl.pallas_call(
            store_kernel,
            out_shape=outs,
            in_specs=[vmem, vmem, vmem],
            out_specs=(hbm, hbm, hbm),
            scratch_shapes=[pltpu.SemaphoreType.DMA((STORES + 2,))],
            compiler_params=pltpu.CompilerParams(vmem_limit_bytes=4 * 2**20),
            name="store",
        )(*(pltpu.with_memory_space_constraint(a, pltpu.VMEM) for a in made))
        return ready, scale, router.T

    return jax.shard_map(
        per_device,
        mesh=mesh,
        in_specs=(P(("unit", "bank"), None, "zero"), P(("unit", "zero"), "bank"), P(("unit", "zero"))),
        out_specs=(P(("unit", "bank"), "zero", None), P(("unit", "bank"), "zero"), P("unit", None)),
        check_vma=False,
    )
```

```python
import functools

import jax
import jax.numpy as jnp
from jax import lax
from jax.experimental import pallas as pl
from jax.experimental.pallas import tpu as pltpu
from jax.sharding import PartitionSpec as P

MESH = pl.DeviceIdType.MESH
LANES = 128
HALF = 8
EARLY = 2
GROUP = 2
TAIL = 4
TIERS = (0, 2, 4)
STORES = 8

PEERS = [(d, c) for c in (1, 0) for d in (4, 3, 5, 2, 6, 1, 7)] + [(0, 1)]
ALIKE = [k for k, (d, c) in enumerate(PEERS) if c == 0]
PARTNER = len(PEERS) - 1
FIRST, SECOND, PEAKS, SCALES, ROUTER, PAIR, PASS, SIDE, WHOLE, BLOCKS = range(10)


def exchange_kernel(
    units,
    x_ref, w_ref, g_ref,
    ready_ref, scale_ref, router_ref,
    xv, wv, gv, sent, early, early_in, early_scale,
    peaks, pair_in, merged, peaks_in, scales, tiles,
    x_sem, send_sem, recv_sem,
):
    chips, banks = units
    experts, rows, _ = x_ref.shape
    per = ready_ref.shape[1]
    me = lax.axis_index("zero")
    chip, core = me // 2, lax.rem(me, 2)
    bank = lax.axis_index("bank")
    mine = pl.ds(pl.multiple_of(me * LANES, LANES), LANES)
    every = range(len(PEERS))

    def peer(k):
        ahead, other = PEERS[k]
        chip_to = lax.rem(chip + ahead, chips)
        core_to = lax.rem(core + other, 2)
        return chip_to, {"zero": chip_to * 2 + core_to}

    def load(e):
        return pltpu.make_async_copy(x_ref.at[e], xv.at[e], x_sem.at[e])

    for e in range(experts):
        load(e).start()
    weight_in = pltpu.make_async_copy(w_ref, wv, x_sem.at[experts])
    gain_in = pltpu.make_async_copy(g_ref, gv, x_sem.at[experts + 1])
    weight_in.start()
    gain_in.start()

    barrier = pltpu.get_barrier_semaphore()
    for k in every:
        pl.semaphore_signal(barrier, inc=1, device_id=peer(k)[1], device_id_type=MESH)
    for b in range(1, banks):
        to = lax.rem(bank + b, banks)
        pl.semaphore_signal(barrier, inc=1, device_id={"bank": to}, device_id_type=MESH)

    def peak(e, block):
        tile = jnp.abs(xv[e, pl.ds(block * LANES, LANES), :])
        return jnp.max(tile.T, axis=0, keepdims=True)

    for e in range(EARLY):
        load(e).wait()
        early[e] = jnp.concatenate([peak(e, b) for b in range(chips)], axis=0)

    def copy(src, dst, kind, k, to=None):
        return pltpu.make_async_remote_copy(
            src_ref=src, dst_ref=dst,
            send_sem=send_sem.at[kind], recv_sem=recv_sem.at[kind],
            device_id=peer(k)[1] if to is None else to, device_id_type=MESH,
        )

    def await_all(ref, sem):
        pltpu.make_async_copy(ref, ref, sem).wait()

    def early_copy(i, k):
        return copy(early.at[i], early_in.at[i, k], FIRST + i, k)

    def peaks_copy(k):
        return copy(merged.at[peer(k)[0]], peaks_in.at[ALIKE.index(k)], PEAKS, k)

    pair_copy = copy(peaks.at[1 - core], pair_in, PAIR, PARTNER)

    def scales_copy(k):
        place = scales.at[core, chip]
        return copy(place, place, SCALES, k)

    scales_pass = copy(scales.at[core], scales.at[core], PASS, PARTNER)
    rank = pl.ds(pl.multiple_of(bank * 16, 16), 16)
    column = pl.ds(pl.multiple_of(chip * LANES, LANES), LANES)
    sevenths = tiles.at[0, pl.ds(0, 16), pl.ds(0, (chips - 1) * LANES)]

    def router_copy(k):
        place = tiles.at[core, rank, column]
        return copy(place, place, ROUTER, k)

    def cross_copy(b):
        place = tiles.at[core, rank]
        return copy(place, place, SIDE, None, {"bank": lax.rem(bank + b, banks)})

    router_pass = copy(tiles.at[core], tiles.at[core], WHOLE, PARTNER)

    def block_copy(e0, n, k):
        to = peer(k)[1]
        experts_of = pl.ds(e0, n)
        return copy(sent.at[to["zero"], experts_of], ready_ref.at[experts_of, :, mine], BLOCKS, k)

    pl.semaphore_wait(barrier, len(PEERS) + banks - 1)
    for i in range(EARLY):
        for k in every:
            early_copy(i, k).start()
    for e in range(EARLY, experts):
        load(e).wait()

    def half_peaks(half):
        @pl.loop(0, chips // 2)
        def _(pair):
            for block in (2 * pair, 2 * pair + 1):
                found = [peak(half * HALF + i, block) for i in range(HALF)]
                peaks[half, block] = jnp.concatenate(found, axis=0)

    half_peaks(1 - core)
    pair_copy.start()
    half_peaks(core)
    pair_copy.wait_recv()
    merged[...] = jnp.maximum(peaks[core], pair_in[...])
    for k in ALIKE:
        peaks_copy(k).start()
    weight_in.wait()
    gain_in.wait()
    tiles[core, rank, column] = (wv[...] * gv[...]).astype(jnp.bfloat16)
    for k in ALIKE:
        router_copy(k).start()

    def scaled(e, row_of):
        for b in range(chips):
            inverse = 1.0 / row_of(b)
            spread = jnp.broadcast_to(inverse, (LANES, LANES)).T
            y = (xv[e, pl.ds(b * LANES, LANES), :] * spread).astype(jnp.bfloat16)
            sent[2 * b, e] = y[:per]
            sent[2 * b + 1, e] = y[per:]
        ready_ref[e, :, mine] = sent[me, e]

    def early_scaled(e):
        await_all(early_in.at[e], recv_sem.at[FIRST + e])
        early_scale[e] = functools.reduce(jnp.maximum, [early_in[e, k] for k in every], early[e])
        scaled(e, lambda b: early_scale[e, b : b + 1, :])

    early_scaled(0)
    for k in every[:10]:
        block_copy(0, 1, k).start()
    await_all(peaks_in, recv_sem.at[PEAKS])
    top = merged[chip]
    for k in ALIKE:
        top = jnp.maximum(top, peaks_in[ALIKE.index(k)])
    scales[core, chip] = top
    for k in ALIKE:
        scales_copy(k).start()
    for k in every[10:]:
        block_copy(0, 1, k).start()
    early_scaled(1)
    for k in every:
        block_copy(1, EARLY - 1, k).start()
    await_all(sevenths, recv_sem.at[ROUTER])
    for b in range(1, banks):
        cross_copy(b).start()
    await_all(peaks_in, recv_sem.at[SCALES])
    scales_pass.start()
    scales_pass.wait_recv()
    def scale_group(e0):
        for j in range(GROUP):
            e = e0 + j
            scaled(e, lambda b: scales[e // HALF, b, pl.ds(lax.rem(e, HALF), 1), :])

    tail = experts - TAIL

    @pl.loop(0, (tail - EARLY) // GROUP)
    def _(i):
        scale_group(EARLY + i * GROUP)
        for k in [PARTNER, *every[:PARTNER]]:
            block_copy(EARLY + i * GROUP, GROUP, k).start()

    pl.loop(0, TAIL // GROUP)(lambda i: scale_group(tail + i * GROUP))

    def tail_blocks(first, past):
        @pl.loop(0, TAIL // GROUP)
        def _(i):
            for k in every:
                to = peer(k)[0]

                @pl.when((to >= first) & (to < past))
                def _():
                    block_copy(tail + i * GROUP, GROUP, k).start()

    for first, past in zip(TIERS, TIERS[1:] + (chips,)):
        tail_blocks(first, past)

    whole = jnp.concatenate([scales[0, chip], scales[1, chip]], axis=0)
    scale_ref[...] = jnp.where(core == 0, whole[:, :per], whole[:, per:])
    await_all(tiles.at[core, pl.ds(0, 16 * (banks - 1))], recv_sem.at[SIDE])
    router_pass.start()
    router_pass.wait()
    for j in range(chips):
        for c in range(2):
            at = (2 * j + c) * LANES
            router_ref[:, at : at + LANES] = tiles[c, :, j * LANES : (j + 1) * LANES]
    for e in range(EARLY):
        await_all(early_in.at[e], send_sem.at[FIRST + e])
    await_all(peaks_in, send_sem.at[PEAKS])
    await_all(peaks_in, send_sem.at[SCALES])
    await_all(sevenths, send_sem.at[ROUTER])
    await_all(tiles.at[core, pl.ds(0, 16 * (banks - 1))], send_sem.at[SIDE])
    pair_copy.wait_send()
    scales_pass.wait_send()
    blocks = sent.at[pl.ds(0, len(PEERS))]
    await_all(blocks, send_sem.at[BLOCKS])
    await_all(blocks, recv_sem.at[BLOCKS])


def store_kernel(ready, scale, router, ready_ref, scale_ref, router_ref, sem):
    step = ready.shape[0] // STORES
    parts = [pl.ds(i * step, step) for i in range(STORES)]
    moves = [(ready.at[p], ready_ref.at[p]) for p in parts]
    moves += [(scale, scale_ref), (router, router_ref)]
    copies = [pltpu.make_async_copy(*m, sem.at[i]) for i, m in enumerate(moves)]
    for c in copies:
        c.start()
    for c in copies:
        c.wait()


def solution(mesh):
    chips, banks = mesh.shape["zero"] // 2, mesh.shape["bank"]

    def per_device(train_down, router_weight, router_gain):
        experts, rows, lanes = train_down.shape
        per = rows // (2 * chips)
        columns = router_weight.shape[1]
        vmem = pl.BlockSpec(memory_space=pltpu.VMEM)
        hbm = pl.BlockSpec(memory_space=pltpu.HBM)
        n = len(PEERS)
        outs = (
            jax.ShapeDtypeStruct((experts, per, 2 * chips * lanes), jnp.bfloat16),
            jax.ShapeDtypeStruct((experts, per), jnp.float32),
            jax.ShapeDtypeStruct((columns * banks, 2 * chips * LANES), jnp.bfloat16),
        )
        held = [
            pltpu.with_memory_space_constraint(a, pltpu.HBM)
            for a in (train_down, router_weight.T, router_gain.reshape(1, -1))
        ]
        made = pl.pallas_call(
            functools.partial(exchange_kernel, (chips, banks)),
            out_shape=outs,
            in_specs=[hbm, hbm, hbm],
            out_specs=(vmem, vmem, vmem),
            scratch_shapes=[
                pltpu.VMEM((experts, rows, lanes), jnp.float32),
                pltpu.VMEM((columns, LANES), jnp.float32),
                pltpu.VMEM((1, LANES), jnp.float32),
                pltpu.VMEM((2 * chips, experts, per, lanes), jnp.bfloat16),
                pltpu.VMEM((EARLY, chips, LANES), jnp.float32),
                pltpu.VMEM((EARLY, n, chips, LANES), jnp.float32),
                pltpu.VMEM((EARLY, chips, LANES), jnp.float32),
                pltpu.VMEM((2, chips, HALF, LANES), jnp.float32),
                pltpu.VMEM((chips, HALF, LANES), jnp.float32),
                pltpu.VMEM((chips, HALF, LANES), jnp.float32),
                pltpu.VMEM((chips - 1, HALF, LANES), jnp.float32),
                pltpu.VMEM((2, chips, HALF, LANES), jnp.float32),
                pltpu.VMEM((2, columns * banks, chips * LANES), jnp.bfloat16),
                pltpu.SemaphoreType.DMA((experts + 2,)),
                pltpu.SemaphoreType.DMA((BLOCKS + 1,)),
                pltpu.SemaphoreType.DMA((BLOCKS + 1,)),
            ],
            compiler_params=pltpu.CompilerParams(
                collective_id=0, has_side_effects=True, vmem_limit_bytes=24 * 2**20
            ),
            name="exchange",
        )(*held)
        ready, scale, router = pl.pallas_call(
            store_kernel,
            out_shape=outs,
            in_specs=[vmem, vmem, vmem],
            out_specs=(hbm, hbm, hbm),
            scratch_shapes=[pltpu.SemaphoreType.DMA((STORES + 2,))],
            compiler_params=pltpu.CompilerParams(vmem_limit_bytes=4 * 2**20),
            name="store",
        )(*(pltpu.with_memory_space_constraint(a, pltpu.VMEM) for a in made))
        return ready, scale, router.T

    return jax.shard_map(
        per_device,
        mesh=mesh,
        in_specs=(P(("unit", "bank"), None, "zero"), P(("unit", "zero"), "bank"), P(("unit", "zero"))),
        out_specs=(P(("unit", "bank"), "zero", None), P(("unit", "bank"), "zero"), P("unit", None)),
        check_vma=False,
    )
```
